128 devices in a mesh: seq: 8 (over z, core), exp: 16 (over y, x).
Axes of the slice: x: 4, y: 4, z: 4, core: 2. Of those that a mesh axis runs over, the one named last changes fastest.
Arguments:
- tokens: bfloat16 [81920, 4096], P(('seq', 'exp')), may hold values from -6 to 6
- routes: int32 [81920, 2], P(('seq', 'exp')), may hold values from 0 to 31, all different within a row; in each aligned block of 640 rows (0 to 639, 640 to 1279, ...) at most 50 rows name the same one
- gates: float32 [81920, 2], P(('seq', 'exp')), may hold values from 0.1 to 1
- weights: bfloat16 [32, 4096, 1024], P('exp', 'seq'), may hold values from -0.09375 to 0.09375
Outputs:
- mixed: bfloat16 [81920, 1024], P(('seq', 'exp'))
The draws below stay inside these ranges and needn't reach their ends.
Inputs may be any that keep to these rules, and one draw needn't show every extreme that they name: `routes`: the two experts of a token differ. Among the rows of one device no expert is named more than 50 times, a bound that some block reaches.
All inputs are finite; a program needn't handle non-finite values.
Results may differ from the reference program's by a relative error of at most 0.0049.
Values may be sent and summed in bfloat16 or wider, within the bound.
A program may use at most 192 MiB of HBM per device.

```python
import math
import jax
import jax.numpy as jnp
import numpy as np
from jax import lax

D = 4096
FF = 1024
TOK_DEV = 640
EXPERTS = 32
CAP = 50
TOKENS = 81920


def levels(rng, shape, shards, low, high):
    factor_of = 1.0
    for dim, shards_of in shards:
        draws = jax.random.uniform(jax.random.fold_in(jax.random.fold_in(rng, 6), dim), (shards_of,), jnp.float32, low / len(shards), high / len(shards))
        factor_of = factor_of * jnp.repeat(jnp.exp(draws), shape[dim] // shards_of).reshape((-1,) + (1,) * (len(shape) - 1 - dim))
    return factor_of


def deal_out(stream_key, own, number, rows, amount, top, limit, slope):
    sequence = jax.random.permutation(stream_key, amount)
    crowded, common = shares(amount, rows * top, limit, slope, True), shares(amount, rows * top, limit, slope, False)
    places = jnp.arange(amount)

    def named(lengths, turn):
        used = int((lengths > 0).sum())
        fixed = max(1, used // 4)
        shifted = fixed + (places - fixed + turn * (used - fixed)) % max(1, amount - fixed)
        return jnp.zeros((amount,), jnp.int32).at[sequence[jnp.where(places < fixed, places, shifted)]].set(jnp.asarray(lengths, jnp.int32))

    lengths = jnp.where(number % 4 == 0, named(crowded, number // 4), named(common, number - number // 4 - 1))
    mixed = jax.random.permutation(jax.random.fold_in(own, 3), amount)
    donor, sink = mixed[0:amount // 2 * 2:2], mixed[1:amount // 2 * 2:2]
    margin = jnp.minimum(lengths[donor] - 1, limit - lengths[sink]) // 2
    margin = jnp.where((donor == sequence[0]) | (sink == sequence[0]) | (lengths[sink] == 0), 0, jnp.maximum(margin, 0))
    shifted = jax.random.randint(jax.random.fold_in(own, 4), (amount // 2,), 0, 1 << 20) % (margin + 1)
    lengths = lengths.at[donor].add(-shifted).at[sink].add(shifted)
    items = jnp.searchsorted(jnp.cumsum(lengths), jnp.arange(rows * top), side="right").astype(jnp.int32)
    grid = items.reshape(top, rows).T
    grid = grid[jax.random.permutation(jax.random.fold_in(own, 1), rows)]
    turn = jax.random.randint(jax.random.fold_in(own, 2), (rows, 1), 0, top)
    return jnp.take_along_axis(grid, (jnp.arange(top)[None, :] + turn) % top, axis=1)


def shares(number_of, total, most, skew, full):
    weights = [(1 << 20) // math.isqrt(standing ** skew) + 1 for standing in range(1, number_of + 1)]
    largest = most if full else min(most, max(-(-total // number_of), total * weights[0] // sum(weights)))
    least = 1 if total - largest >= number_of - 1 else 0
    holding, rest = [largest] + [least] * (number_of - 1), total - largest - least * (number_of - 1)
    while rest > 0:
        free = [i for i in range(1, number_of) if holding[i] < largest] or [i for i in range(1, number_of) if holding[i] < most]
        mass, budget = sum([weights[i] for i in free]), rest
        for i in free:
            more = min(most - holding[i], max(1, budget * weights[i] // mass), rest)
            holding[i] = holding[i] + more
            rest = rest - more
    return np.array(holding)


def scatter_about(rng, extent, scale, most, pieces=(), held_as=jnp.bfloat16):
    gain = levels(rng, extent, pieces, -0.22, 0.18) if pieces else 1.0
    drawn = jax.random.normal(rng, extent, jnp.float32) * scale * gain
    return jnp.minimum(jnp.maximum(drawn, -most), most).astype(held_as)


def setup_inputs(seed: int = 0) -> dict:
    seeds = jax.random.split(jax.random.key(seed), 5)
    tokens = scatter_about(seeds[0], (TOKENS, D), 1.0, 6.0, ((0, 128),))
    routes_keys = jax.random.split(jax.random.fold_in(seeds[1], 1), TOKENS // TOK_DEV)
    routes_turns = jax.random.permutation(jax.random.fold_in(seeds[1], 3), TOKENS // TOK_DEV)
    routes = jax.vmap(lambda own, number: deal_out(jax.random.fold_in(seeds[1], 2), own, number, TOK_DEV, EXPERTS, 2, CAP, 2))(routes_keys, routes_turns).reshape((TOKENS, 2))
    gates = jnp.clip(0.1 + 0.9 * jax.random.uniform(seeds[2], (TOKENS, 2), jnp.float32) ** levels(seeds[2], (TOKENS, 2), ((0, 128),), -0.2, 0.2), 0.1, 1.0)
    weights = scatter_about(seeds[3], (EXPERTS, D, FF), D ** -0.5, 0.09375, ((0, 16), (1, 8)))
    return dict(tokens=tokens, routes=routes, gates=gates, weights=weights)


def route_slots(route_block, experts, capacity):
    expert_ids = route_block.reshape(-1)
    one_hot = (expert_ids[:, None] == jnp.arange(experts, dtype=jnp.int32)[None, :]).astype(jnp.int32)
    earlier = jnp.cumsum(one_hot, axis=0) - one_hot
    slot_index = jnp.sum(earlier * one_hot, axis=1)
    return (expert_ids * capacity + slot_index).astype(jnp.int32)


def reference(tokens, routes, gates, weights):
    blocks = TOKENS // TOK_DEV
    route_blocks = routes.reshape(blocks, TOK_DEV, 2)
    position = jax.vmap(lambda block: route_slots(block, EXPERTS, CAP))(route_blocks)
    local_rows = jnp.arange(2 * TOK_DEV, dtype=jnp.int32) // 2
    block_base = (jnp.arange(blocks, dtype=jnp.int32) * TOK_DEV)[:, None]
    global_rows = block_base + local_rows[None, :]

    def fill_table(places, rows):
        return jnp.full((EXPERTS * CAP,), TOKENS, jnp.int32).at[places].set(rows)

    slot_rows = jax.vmap(fill_table)(position, global_rows).reshape(blocks, EXPERTS, CAP)
    padded = jnp.concatenate([tokens, jnp.zeros((1, D), jnp.bfloat16)], axis=0)

    def one_expert(expert):
        indices = lax.dynamic_index_in_dim(slot_rows, expert, 1, keepdims=False).reshape(-1)
        gathered = padded[indices]
        matrix = lax.dynamic_index_in_dim(weights, expert, 0, keepdims=False)
        return jnp.dot(gathered, matrix, preferred_element_type=jnp.float32).astype(jnp.bfloat16)

    outputs = lax.map(one_expert, jnp.arange(EXPERTS, dtype=jnp.int32))
    outputs = outputs.reshape(EXPERTS * blocks * CAP, FF)
    expert_ids = route_blocks.reshape(blocks, 2 * TOK_DEV)
    slot_index = position - expert_ids * CAP
    block_ids = jnp.arange(blocks, dtype=jnp.int32)[:, None]
    flat_index = ((expert_ids * blocks + block_ids) * CAP + slot_index).reshape(-1)
    picked = outputs[flat_index].reshape(TOKENS, 2, FF).astype(jnp.float32)
    mixed = jnp.sum(picked * gates[:, :, None], axis=1)
    return mixed.astype(jnp.bfloat16)
```

```python
import functools

import jax
import jax.numpy as jnp
from jax import lax
from jax.experimental import pallas as pl
from jax.experimental.pallas import tpu as pltpu
from jax.sharding import PartitionSpec as P

GROUP = 4
TILE = 8


def shift_order(side):
    if side == 4:
        return [
            (2, 2), (1, 1), (3, 3), (2, 0),
            (1, 2), (3, 2), (2, 1), (0, 3),
            (2, 3), (1, 3), (3, 1), (0, 2),
            (1, 0), (3, 0), (0, 1), (0, 0),
        ]
    all_shifts = [(a, b) for a in range(side) for b in range(side)]
    return all_shifts[1:] + all_shifts[:1]


def kernel(side, depth_z, cap, tok, routes, routes_t, gates, w, out,
           send, recv, wfull, rr, oh, xbuf, acc,
           xsem, tsend, trecv, rsend, rrecv, wloc, wsend, wrecv):
    count, width = tok.shape
    hidden = w.shape[2]
    shard = w.shape[1]
    peers = side * side
    rows = 2 * cap
    padded = send.shape[1]
    experts = 2 * peers
    sent = -(-rows // TILE) * TILE
    groups = peers // GROUP
    chunks = 4
    chunk = width // chunks
    f32, bf16 = jnp.float32, jnp.bfloat16

    seq = lax.axis_index("seq")
    exp = lax.axis_index("exp")
    z, core = seq // 2, lax.rem(seq, 2)
    y, x = exp // side, lax.rem(exp, side)
    sibling = 2 * z + 1 - core
    shifts = shift_order(side)

    def there(i):
        return lax.rem(y + shifts[i][0], side) * side + lax.rem(x + shifts[i][1], side)

    def back(i):
        return (lax.rem(y - shifts[i][0] + side, side) * side
                + lax.rem(x - shifts[i][1] + side, side))

    def z_peer(dz):
        return 2 * lax.rem(z + dz, depth_z) + core

    own_rows = pl.ds(pl.multiple_of(seq * shard, shard), shard)
    local_w = pltpu.make_async_copy(w, wfull.at[:, own_rows, :], wloc)
    local_w.start()

    def x_copy(c):
        return pltpu.make_async_copy(
            tok.at[:, pl.ds(c * chunk, chunk)], xbuf.at[c % 2], xsem.at[c % 2])

    x_copy(0).start()
    x_copy(1).start()

    barrier = pltpu.get_barrier_semaphore()
    for i in range(peers - 1):
        pl.semaphore_signal(barrier, inc=1, device_id={"exp": there(i)})
    for dz in range(1, depth_z):
        pl.semaphore_signal(barrier, inc=1, device_id={"seq": z_peer(dz)})
    pl.semaphore_signal(barrier, inc=1, device_id={"seq": sibling})

    ra, rb = routes_t[0:1, :], routes_t[1:2, :]
    names = lax.broadcasted_iota(jnp.int32, (experts, count), 0)
    hit_a, hit_b = names == ra, names == rb
    both = jnp.where(hit_a | hit_b, 1.0, 0.0).astype(bf16)
    earlier = jnp.where(
        lax.broadcasted_iota(jnp.int32, (count, count), 0)
        < lax.broadcasted_iota(jnp.int32, (count, count), 1), 1.0, 0.0).astype(bf16)
    table = (jnp.dot(both, earlier, preferred_element_type=f32)
             + (names * cap).astype(f32))
    pos_a = jnp.sum(jnp.where(hit_a, table, 0.0), axis=0, keepdims=True)
    pos_b = jnp.sum(jnp.where(hit_b, table, 0.0), axis=0, keepdims=True)

    for i in range(peers):
        r = lax.broadcasted_iota(jnp.int32, (padded, count), 0)
        target = jnp.where(r < rows, (r + rows * there(i)), -1).astype(f32)
        hit = (pos_a == target) | (pos_b == target)
        oh[i * padded:(i + 1) * padded, :] = jnp.where(hit, 1.0, 0.0).astype(bf16)

    pl.semaphore_wait(barrier, peers - 1 + depth_z - 1 + 1)

    def w_copy(n, zo, co, src, target):
        span = pl.ds(pl.multiple_of((2 * zo + co) * shard, shard), shard)
        return pltpu.make_async_remote_copy(
            src_ref=src if src is not None else wfull.at[:, span, :],
            dst_ref=wfull.at[:, span, :],
            send_sem=wsend.at[n], recv_sem=wrecv.at[n],
            device_id={"seq": target})

    for dz in range(1, depth_z):
        w_copy(dz, z, core, w, z_peer(dz)).start()
    w_copy(depth_z, z, core, w, sibling).start()

    def t_copy(i, c):
        cols = pl.ds(0, width) if c is None else pl.ds(c * chunk, chunk)
        return pltpu.make_async_remote_copy(
            src_ref=send.at[i, pl.ds(0, sent), cols],
            dst_ref=recv.at[i, pl.ds(0, sent), cols],
            send_sem=tsend.at[i, 0 if c is None else c],
            recv_sem=trecv.at[i, 0 if c is None else c],
            device_id={"exp": there(i)})

    for c in range(chunks):
        x_copy(c).wait()
        for g in range(groups):
            got = jnp.dot(oh[g * GROUP * padded:(g + 1) * GROUP * padded, :], xbuf[c % 2],
                          preferred_element_type=f32).astype(bf16)
            got = got.reshape(GROUP, padded, chunk)
            cols = slice(c * chunk, (c + 1) * chunk)
            if g < groups - 1:
                send[g * GROUP:(g + 1) * GROUP, :, cols] = got
            else:
                send[g * GROUP:g * GROUP + GROUP - 1, :, cols] = got[:GROUP - 1]
                recv[peers - 1, :, cols] = got[GROUP - 1]
            if g == 0:
                for i in range(GROUP):
                    t_copy(i, c).start()
            elif c == chunks - 1:
                for i in range(g * GROUP, min((g + 1) * GROUP, peers - 1)):
                    t_copy(i, None).start()
        if c + 2 < chunks:
            x_copy(c + 2).start()

    local_w.wait()
    for dz in [d for d in (1, 3, 2) if d < depth_z]:
        zo = lax.rem(z - dz + depth_z, depth_z)
        w_copy(dz, zo, core, None, seq).wait_recv()
        w_copy(depth_z + dz, zo, core, None, sibling).start()
    for dz in range(depth_z):
        zo = lax.rem(z - dz + depth_z, depth_z)
        w_copy(depth_z + dz, zo, 1 - core, None, sibling).wait_recv()

    def r_copy(i):
        return pltpu.make_async_remote_copy(
            src_ref=send.at[i, pl.ds(0, sent), pl.ds(0, hidden)],
            dst_ref=rr.at[i, pl.ds(0, sent), :],
            send_sem=rsend.at[i], recv_sem=rrecv.at[i],
            device_id={"exp": back(i)})

    def members(g):
        return range(g * GROUP, min((g + 1) * GROUP, peers - 1))

    step = min(256, hidden)
    for g in range(groups):
        for i in members(g):
            for c in range(chunks if g == 0 else 1):
                copy = t_copy(i, c if g == 0 else None)
                copy.wait_send()
                copy.wait_recv()

        def product(n, carry, g=g):
            cols = pl.ds(pl.multiple_of(n * step, step), step)
            left = recv[g * GROUP:(g + 1) * GROUP].reshape(GROUP * padded, width)
            first = jnp.dot(left, wfull[0, :, cols], preferred_element_type=f32)
            second = jnp.dot(left, wfull[1, :, cols], preferred_element_type=f32)
            first = first.reshape(GROUP, padded, step)
            second = second.reshape(GROUP, padded, step)
            r = lax.broadcasted_iota(jnp.int32, (GROUP, padded, step), 1)
            both = jnp.where(r < cap, first, second).astype(bf16)
            if g < groups - 1:
                send[g * GROUP:(g + 1) * GROUP, :, cols] = both
            else:
                send[g * GROUP:g * GROUP + GROUP - 1, :, cols] = both[:GROUP - 1]
                rr[peers - 1, :, cols] = both[GROUP - 1]
            return carry

        lax.fori_loop(0, hidden // step, product, 0)
        for i in members(g):
            r_copy(i).start()

    ra, rb = routes[:, 0:1], routes[:, 1:2]
    lanes = max(experts, 128)
    names = lax.broadcasted_iota(jnp.int32, (count, lanes), 1)
    hit_a, hit_b = names == ra, names == rb
    both = jnp.where(hit_a | hit_b, 1.0, 0.0).astype(bf16)
    earlier = jnp.where(
        lax.broadcasted_iota(jnp.int32, (count, count), 1)
        < lax.broadcasted_iota(jnp.int32, (count, count), 0), 1.0, 0.0).astype(bf16)
    table = (jnp.dot(earlier, both, preferred_element_type=f32)
             + (names * cap).astype(f32))
    pos_a = jnp.sum(jnp.where(hit_a, table, 0.0), axis=1, keepdims=True)
    pos_b = jnp.sum(jnp.where(hit_b, table, 0.0), axis=1, keepdims=True)
    gate_a, gate_b = gates[:, 0:1], gates[:, 1:2]

    for g in range(groups):
        lane = lax.broadcasted_iota(jnp.int32, (1, GROUP * padded), 1)
        target = jnp.full_like(lane, -1)
        for j in range(GROUP):
            r = lane - j * padded
            target = jnp.where((r >= 0) & (r < rows), r + rows * there(g * GROUP + j), target)
        target = target.astype(f32)
        mix = jnp.where(pos_a == target, gate_a, 0.0) + jnp.where(pos_b == target, gate_b, 0.0)
        high = mix.astype(bf16)
        low = (mix - high.astype(f32)).astype(bf16)
        for i in members(g):
            r_copy(i).wait_recv()
        right = rr[g * GROUP:(g + 1) * GROUP]
        r = lax.broadcasted_iota(jnp.int32, right.shape, 1)
        right = jnp.where(r < rows, right, jnp.zeros_like(right))
        right = right.reshape(GROUP * padded, hidden)
        part = (jnp.dot(high, right, preferred_element_type=f32)
                + jnp.dot(low, right, preferred_element_type=f32))
        if g == 0:
            acc[...] = part
        elif g < groups - 1:
            acc[...] += part
        else:
            out[...] = (acc[...] + part).astype(bf16)

    for i in range(peers - 1):
        r_copy(i).wait_send()
    for dz in range(1, depth_z):
        w_copy(dz, z, core, w, z_peer(dz)).wait_send()
    w_copy(depth_z, z, core, w, sibling).wait_send()
    for dz in range(1, depth_z):
        zo = lax.rem(z - dz + depth_z, depth_z)
        w_copy(depth_z + dz, zo, core, None, sibling).wait_send()


def body(side, depth_z, tokens, routes, gates, weights):
    peers = side * side
    count, width = tokens.shape
    hidden = weights.shape[2]
    cap = 5 * count // (4 * peers)
    rows = 2 * cap
    padded = -(-rows // 16) * 16
    bf16 = jnp.bfloat16
    dma = pltpu.SemaphoreType.DMA
    vmem = pl.BlockSpec(memory_space=pltpu.VMEM)
    anywhere = pl.BlockSpec(memory_space=pl.ANY)
    return pl.pallas_call(
        functools.partial(kernel, side, depth_z, cap),
        out_shape=jax.ShapeDtypeStruct((count, hidden), bf16),
        in_specs=[anywhere, vmem, vmem, vmem, anywhere],
        out_specs=vmem,
        scratch_shapes=[
            pltpu.VMEM((peers - 1, padded, width), bf16),
            pltpu.VMEM((peers, padded, width), bf16),
            pltpu.VMEM((2, width, hidden), bf16),
            pltpu.VMEM((peers, padded, hidden), bf16),
            pltpu.VMEM((peers * padded, count), bf16),
            pltpu.VMEM((2, count, width // 4), bf16),
            pltpu.VMEM((count, hidden), jnp.float32),
            dma((2,)),
            dma((peers, 4)),
            dma((peers, 4)),
            dma((peers,)),
            dma((peers,)),
            dma,
            dma((2 * depth_z,)),
            dma((2 * depth_z,)),
        ],
        compiler_params=pltpu.CompilerParams(
            collective_id=0, has_side_effects=True, vmem_limit_bytes=67043328),
    )(tokens, routes, routes.T, gates, weights)


def solution(mesh):
    side = {4: 2, 16: 4}[mesh.shape["exp"]]
    return jax.shard_map(
        functools.partial(body, side, mesh.shape["seq"] // 2),
        mesh=mesh,
        in_specs=(
            P(("seq", "exp"), None),
            P(("seq", "exp"), None),
            P(("seq", "exp"), None),
            P("exp", "seq", None),
        ),
        out_specs=P(("seq", "exp"), None),
        check_vma=False,
    )
```

```python
import functools

import jax
import jax.numpy as jnp
from jax import lax
from jax.experimental import pallas as pl
from jax.experimental.pallas import tpu as pltpu
from jax.sharding import PartitionSpec as P

SIDE = 4
DEPTH = 4
GROUP = 4
TILE = 8
SENDS = [("b", 2), ("d", 2), ("b", 1), ("d", 1), ("b", 3), ("d", 3), ("b", 0), ("d", 0),
         ("a", 2), ("c", 2), ("a", 1), ("c", 1), ("a", 3), ("c", 3), ("a", 0), ("c", 0)]
SLOTS = [("a", 0), ("b", 0), ("a", 2), ("a", 1), ("a", 3), ("b", 2), ("b", 1), ("b", 3),
         ("c", 0), ("d", 0), ("c", 2), ("c", 1), ("c", 3), ("d", 2), ("d", 1), ("d", 3)]
SELF = [("a", 0), ("c", 0)]
RELAYED = [("b", 2), ("d", 2), ("b", 1), ("d", 1), ("b", 3), ("d", 3)]


def flip(v):
    return v + 1 - 2 * lax.rem(v, 2)


def choose(v, parity, even, odd):
    return even + (odd - even) * lax.rem(parity, 2)


def mate(v, parity):
    return choose(v, parity, flip(v), SIDE - 1 - v)


def beside(v, parity):
    return choose(v, parity, SIDE - 1 - v, flip(v))


def kernel(cap, tok, routes, routes_t, gates, w, out, held,
           send, recv, land, res, rr_lo, rr_hi, oh, xbuf, wbuf, acc, pos,
           xsem, wbsem, tsend, trecv, usend, urecv, lsend, lrecv, hsend, hrecv,
           wloc, wsend, wrecv):
    count, width = tok.shape
    shard, hidden = w.shape[1:]
    rows = 2 * cap
    padded = recv.shape[1]
    sent = -(-rows // TILE) * TILE
    low_rows = cap // 16 * 16
    span = padded - low_rows
    peers = SIDE * SIDE
    experts = 2 * peers
    chunks = 4
    chunk = width // chunks
    f32, bf16 = jnp.float32, jnp.bfloat16

    seq = lax.axis_index("seq")
    exp = lax.axis_index("exp")
    z, core = seq // 2, lax.rem(seq, 2)
    y, x = exp // SIDE, lax.rem(exp, SIDE)
    sibling = 2 * z + 1 - core

    def turn(v, d):
        return lax.rem(v + d + SIDE, SIDE)

    def place(yy, xx):
        return yy * SIDE + xx

    def goal(m):
        kind, d = m
        if kind == "a":
            yy, xx = turn(y, d), x
        elif kind == "b":
            yy = turn(y, d)
            xx = beside(x, yy)
        elif kind == "c":
            yy, xx = y, turn(x, d)
        else:
            xx = turn(x, d)
            yy = beside(y, xx)
        if kind in "ab":
            return (yy, xx), (yy, mate(xx, yy)), 0
        return (yy, xx), (mate(yy, xx), xx), 1

    def corner(m):
        kind, d = m
        if kind == "b":
            return place(y, beside(x, turn(y, d)))
        if kind == "d":
            return place(beside(y, turn(x, d)), x)
        return place(*goal(m)[0])

    def origin(m):
        kind, d = m
        if kind == "a":
            return place(turn(y, -d), x)
        if kind == "b":
            return place(turn(y, -d), beside(x, y))
        if kind == "c":
            return place(y, turn(x, -d))
        return place(beside(y, x), turn(x, -d))

    def names_of(m):
        first, second, which = goal(m)
        return 2 * place(*first) + which, 2 * place(*second) + which

    def rows_of(zz, cc):
        return pl.ds(pl.multiple_of((2 * zz + cc) * shard, shard), shard)

    local_w = pltpu.make_async_copy(w, held.at[pl.ds(0, 2), rows_of(z, core), :], wloc)
    local_w.start()

    def x_copy(c):
        return pltpu.make_async_copy(
            tok.at[:, pl.ds(c * chunk, chunk)], xbuf.at[c % 2], xsem.at[c % 2])

    x_copy(0).start()
    x_copy(1).start()

    barrier = pltpu.get_barrier_semaphore()
    for i in range(1, peers):
        pl.semaphore_signal(barrier, inc=1, device_id={"exp": lax.rem(exp + i, peers)})
    up, down = 2 * lax.rem(z + 1, DEPTH) + core, 2 * lax.rem(z + DEPTH - 1, DEPTH) + core
    for other in (up, down, sibling):
        pl.semaphore_signal(barrier, inc=1, device_id={"seq": other})

    ra, rb = routes_t[0:1, :], routes_t[1:2, :]
    names = lax.broadcasted_iota(jnp.int32, (experts, count), 0)
    hit_a, hit_b = names == ra, names == rb
    both = jnp.where(hit_a | hit_b, 1.0, 0.0).astype(bf16)
    earlier = jnp.where(
        lax.broadcasted_iota(jnp.int32, (count, count), 0)
        < lax.broadcasted_iota(jnp.int32, (count, count), 1), 1.0, 0.0).astype(bf16)
    table = (jnp.dot(both, earlier, preferred_element_type=f32)
             + (names * cap).astype(f32))
    pos_a = jnp.sum(jnp.where(hit_a, table, 0.0), axis=0, keepdims=True)
    pos_b = jnp.sum(jnp.where(hit_b, table, 0.0), axis=0, keepdims=True)

    for i, m in enumerate(SENDS):
        e1, e2 = names_of(m)
        r = lax.broadcasted_iota(jnp.int32, (padded, count), 0)
        target = jnp.where(r < cap, r + e1 * cap, r - cap + e2 * cap)
        target = jnp.where(r < rows, target, -1).astype(f32)
        hit = (pos_a == target) | (pos_b == target)
        oh[i * padded:(i + 1) * padded, :] = jnp.where(hit, 1.0, 0.0).astype(bf16)

    pl.semaphore_wait(barrier, peers - 1 + 3)

    prev, after, far = turn(z, -1), turn(z, 1), turn(z, 2)

    def w_copy(n, part, zz, cc, expert, many, target, mine=False):
        dst = held.at[pl.ds(expert, many), rows_of(zz, cc), :]
        return pltpu.make_async_remote_copy(
            src_ref=w if mine else dst, dst_ref=dst,
            send_sem=wsend.at[10 * part + n], recv_sem=wrecv.at[10 * part + n],
            device_id={"seq": target})

    def swap(j):
        target = place(y, mate(x, y)) if j == 0 else place(mate(y, x), x)
        return pltpu.make_async_remote_copy(
            src_ref=w.at[pl.ds(j, 1)], dst_ref=held.at[pl.ds(2 + j, 1), rows_of(z, core), :],
            send_sem=wsend.at[20 + j], recv_sem=wrecv.at[20 + j], device_id={"exp": target})

    def w_up(p):
        return w_copy(0, p, z, core, 2 * p, 2, up, mine=p == 0)

    def w_down(p):
        return w_copy(1, p, z, core, 2 * p, 2, down, mine=p == 0)

    def w_up_far(p):
        return w_copy(2, p, prev, core, 2 * p, 1, up)

    def w_down_far(p):
        return w_copy(3, p, after, core, 2 * p + 1, 1, down)

    def w_side(p, n, cc):
        zz, expert, many = [(z, 2 * p, 2), (prev, 2 * p, 2), (after, 2 * p, 2),
                            (far, 2 * p, 1), (far, 2 * p + 1, 1)][n]
        return w_copy(4 + n, p, zz, cc, expert, many, sibling, mine=(p == 0 and n == 0 and cc is core))

    def got(copy_n, p):
        zz, expert, many = [(prev, 2 * p, 2), (after, 2 * p, 2), (far, 2 * p, 1), (far, 2 * p + 1, 1)][copy_n]
        w_copy(copy_n, p, zz, core, expert, many, up).wait_recv()

    w_up(0).start()
    w_down(0).start()
    swap(0).start()
    swap(1).start()
    w_side(0, 0, core).start()

    def t_copy(m, c):
        i = SENDS.index(m)
        cols = pl.ds(0, width) if c is None else pl.ds(c * chunk, chunk)
        if m in RELAYED:
            dst = land.at[RELAYED.index(m), pl.ds(0, sent), cols]
        else:
            dst = recv.at[SLOTS.index(m), pl.ds(0, sent), cols]
        k = 0 if c is None else c
        return pltpu.make_async_remote_copy(
            src_ref=send.at[i, pl.ds(0, sent), cols], dst_ref=dst,
            send_sem=tsend.at[i, k], recv_sem=trecv.at[i, k], device_id={"exp": corner(m)})

    def pieces(m):
        return range(chunks) if SENDS.index(m) < GROUP else [None]

    def u_copy(m):
        kind, d = m
        target = place(turn(y, d), x) if kind == "b" else place(y, turn(x, d))
        i = RELAYED.index(m)
        return pltpu.make_async_remote_copy(
            src_ref=land.at[i, pl.ds(0, sent), :],
            dst_ref=recv.at[SLOTS.index(m), pl.ds(0, sent), :],
            send_sem=usend.at[i], recv_sem=urecv.at[i], device_id={"exp": target})

    groups = peers // GROUP
    for c in range(chunks):
        x_copy(c).wait()
        cols = slice(c * chunk, (c + 1) * chunk)
        for g in range(groups):
            got_rows = jnp.dot(oh[g * GROUP * padded:(g + 1) * GROUP * padded, :], xbuf[c % 2],
                               preferred_element_type=f32).astype(bf16)
            got_rows = got_rows.reshape(GROUP, padded, chunk)
            ms = SENDS[g * GROUP:(g + 1) * GROUP]
            if g < groups - 1:
                send[g * GROUP:(g + 1) * GROUP, :, cols] = got_rows
            else:
                for j, m in enumerate(ms):
                    if m in SELF:
                        recv[SLOTS.index(m), :, cols] = got_rows[j]
                    else:
                        send[g * GROUP + j, :, cols] = got_rows[j]
            for m in ms:
                if m in SELF:
                    continue
                if g == 0:
                    t_copy(m, c).start()
                elif c == chunks - 1:
                    t_copy(m, None).start()
        if c + 2 < chunks:
            x_copy(c + 2).start()

    def landed(m):
        for c in pieces(m):
            t_copy(m, c).wait_recv()

    def relay(m):
        landed(m)
        u_copy(m).start()

    for m in RELAYED[:4]:
        relay(m)

    local_w.wait()
    got(0, 0)
    w_up_far(0).start()
    got(1, 0)
    w_down_far(0).start()
    swap(0).wait_recv()
    swap(1).wait_recv()
    w_up(1).start()
    w_down(1).start()
    w_side(0, 1, core).start()
    w_side(0, 2, core).start()
    w_side(1, 0, core).start()
    for m in RELAYED[4:]:
        relay(m)

    ra, rb = routes[:, 0:1], routes[:, 1:2]
    lanes = max(experts, 128)
    names = lax.broadcasted_iota(jnp.int32, (count, lanes), 1)
    hit_a, hit_b = names == ra, names == rb
    both = jnp.where(hit_a | hit_b, 1.0, 0.0).astype(bf16)
    earlier = jnp.where(
        lax.broadcasted_iota(jnp.int32, (count, count), 1)
        < lax.broadcasted_iota(jnp.int32, (count, count), 0), 1.0, 0.0).astype(bf16)
    table = (jnp.dot(earlier, both, preferred_element_type=f32)
             + (names * cap).astype(f32))
    pos[:, 0:1] = jnp.sum(jnp.where(hit_a, table, 0.0), axis=1, keepdims=True)
    pos[:, 1:2] = jnp.sum(jnp.where(hit_b, table, 0.0), axis=1, keepdims=True)

    got(2, 0)
    w_side(0, 3, core).start()
    got(3, 0)
    w_side(0, 4, core).start()
    for n in range(5):
        w_side(0, n, 1 - core).wait_recv()

    step = wbuf.shape[2]

    def w_load(q, n, slot):
        cols = pl.ds(pl.multiple_of(n * step, step), step)
        return pltpu.make_async_copy(held.at[q, :, cols], wbuf.at[slot], wbsem.at[slot])

    def product(base, q, half):
        start = 0 if half == 0 else low_rows
        w_load(q, 0, 0).start()

        def one(n, carry):
            slot = lax.rem(n, 2)
            w_load(q, n, slot).wait()

            @pl.when(n + 1 < hidden // step)
            def _():
                w_load(q, n + 1, 1 - slot).start()

            cols = pl.ds(pl.multiple_of(n * step, step), step)
            left = recv[base:base + GROUP, start:start + span, :].reshape(GROUP * span, width)
            prod = jnp.dot(left, wbuf[slot], preferred_element_type=f32).astype(bf16)
            prod = prod.reshape(GROUP, span, step)
            if half == 0:
                res[base:base + GROUP, 0:span, cols] = prod
            else:
                edge = res[base:base + GROUP, low_rows:low_rows + 16, cols]
                r = lax.broadcasted_iota(jnp.int32, edge.shape, 1)
                res[base:base + GROUP, low_rows:low_rows + 16, cols] = jnp.where(
                    r < cap - low_rows, edge, prod[:, 0:16])
                res[base:base + GROUP, low_rows + 16:padded, cols] = prod[:, 16:]
            return carry

        lax.fori_loop(0, hidden // step, one, 0)

    def low_copy(m):
        i = SLOTS.index(m)
        return pltpu.make_async_remote_copy(
            src_ref=res.at[i, pl.ds(0, low_rows), :], dst_ref=rr_lo.at[i],
            send_sem=lsend.at[i], recv_sem=lrecv.at[i], device_id={"exp": origin(m)})

    def high_copy(m):
        i = SLOTS.index(m)
        return pltpu.make_async_remote_copy(
            src_ref=res.at[i, pl.ds(low_rows, sent - low_rows), :],
            dst_ref=rr_hi.at[i, pl.ds(0, sent - low_rows), :],
            send_sem=hsend.at[i], recv_sem=hrecv.at[i], device_id={"exp": origin(m)})

    def arrived(m):
        if m in SELF:
            return
        if m in RELAYED:
            u_copy(m).wait_recv()
        else:
            landed(m)

    def give_low(base):
        for i in range(base, base + GROUP):
            if SLOTS[i] in SELF:
                rr_lo[i] = res[i, 0:low_rows, :]
            else:
                low_copy(SLOTS[i]).start()

    def give_high(base):
        for i in range(base, base + GROUP):
            if SLOTS[i] in SELF:
                rr_hi[i] = res[i, low_rows:padded, :]
            else:
                high_copy(SLOTS[i]).start()

    for base, q in ((0, 0), (8, 1)):
        for m in SLOTS[base:base + GROUP]:
            arrived(m)
        product(base, q, 0)
        give_low(base)

    got(0, 1)
    w_up_far(1).start()
    got(1, 1)
    w_down_far(1).start()
    w_side(1, 1, core).start()
    w_side(1, 2, core).start()

    for base, q in ((4, 0), (12, 1)):
        for m in SLOTS[base:base + GROUP]:
            arrived(m)
        product(base, q, 0)
        give_low(base)

    got(2, 1)
    w_side(1, 3, core).start()
    got(3, 1)
    w_side(1, 4, core).start()
    for n in range(5):
        w_side(1, n, 1 - core).wait_recv()

    for base, q in ((0, 2), (8, 3), (4, 2), (12, 3)):
        product(base, q, 1)
        give_high(base)

    gate_a, gate_b = gates[:, 0:1], gates[:, 1:2]
    pos_a, pos_b = pos[:, 0:1], pos[:, 1:2]

    def mixed(base, high):
        size = span if high else low_rows
        lane = lax.broadcasted_iota(jnp.int32, (1, GROUP * size), 1)
        target = jnp.full_like(lane, -1)
        for j in range(GROUP):
            e1, e2 = names_of(SLOTS[base + j])
            local = lane - j * size
            r = local + (low_rows if high else 0)
            value = jnp.where(r < cap, r + e1 * cap, r - cap + e2 * cap)
            target = jnp.where((local >= 0) & (local < size) & (r < rows), value, target)
        target = target.astype(f32)
        mix = jnp.where(pos_a == target, gate_a, 0.0) + jnp.where(pos_b == target, gate_b, 0.0)
        top = mix.astype(bf16)
        rest = (mix - top.astype(f32)).astype(bf16)
        for m in SLOTS[base:base + GROUP]:
            if m not in SELF:
                (high_copy(m) if high else low_copy(m)).wait_recv()
        if high:
            right = rr_hi[base:base + GROUP]
            r = lax.broadcasted_iota(jnp.int32, right.shape, 1)
            right = jnp.where(r < rows - low_rows, right, jnp.zeros_like(right))
        else:
            right = rr_lo[base:base + GROUP]
        right = right.reshape(GROUP * size, hidden)
        return (jnp.dot(top, right, preferred_element_type=f32)
                + jnp.dot(rest, right, preferred_element_type=f32))

    order = [(0, False), (8, False), (4, False), (12, False),
             (0, True), (8, True), (4, True), (12, True)]
    for k, (base, high) in enumerate(order):
        part = mixed(base, high)
        if k == 0:
            acc[...] = part
        elif k < len(order) - 1:
            acc[...] += part
        else:
            out[...] = (acc[...] + part).astype(bf16)

    for m in SENDS:
        if m not in SELF:
            for c in pieces(m):
                t_copy(m, c).wait_send()
            low_copy(m).wait_send()
            high_copy(m).wait_send()
    for m in RELAYED:
        u_copy(m).wait_send()
    swap(0).wait_send()
    swap(1).wait_send()
    for p in range(2):
        for copy in (w_up(p), w_down(p), w_up_far(p), w_down_far(p)):
            copy.wait_send()
        for n in range(5):
            w_side(p, n, core).wait_send()


def body(tokens, routes, gates, weights):
    peers = SIDE * SIDE
    count, width = tokens.shape
    shard, hidden = weights.shape[1:]
    cap = 5 * count // (4 * peers)
    rows = 2 * cap
    padded = -(-rows // 16) * 16
    low_rows = cap // 16 * 16
    span = padded - low_rows
    bf16 = jnp.bfloat16
    dma = pltpu.SemaphoreType.DMA
    vmem = pl.BlockSpec(memory_space=pltpu.VMEM)
    anywhere = pl.BlockSpec(memory_space=pl.ANY)
    step = min(256, hidden)
    mixed, _ = pl.pallas_call(
        functools.partial(kernel, cap),
        out_shape=(
            jax.ShapeDtypeStruct((count, hidden), bf16),
            jax.ShapeDtypeStruct((4, width, hidden), bf16),
        ),
        in_specs=[anywhere, vmem, vmem, vmem, anywhere],
        out_specs=(vmem, anywhere),
        scratch_shapes=[
            pltpu.VMEM((peers - 2, padded, width), bf16),
            pltpu.VMEM((peers, padded, width), bf16),
            pltpu.VMEM((len(RELAYED), padded, width), bf16),
            pltpu.VMEM((peers, padded, hidden), bf16),
            pltpu.VMEM((peers, low_rows, hidden), bf16),
            pltpu.VMEM((peers, span, hidden), bf16),
            pltpu.VMEM((peers * padded, count), bf16),
            pltpu.VMEM((2, count, width // 4), bf16),
            pltpu.VMEM((2, width, step), bf16),
            pltpu.VMEM((count, hidden), jnp.float32),
            pltpu.VMEM((count, 128), jnp.float32),
            dma((2,)),
            dma((2,)),
            dma((peers, 4)),
            dma((peers, 4)),
            dma((len(RELAYED),)),
            dma((len(RELAYED),)),
            dma((peers,)),
            dma((peers,)),
            dma((peers,)),
            dma((peers,)),
            dma,
            dma((22,)),
            dma((22,)),
        ],
        compiler_params=pltpu.CompilerParams(
            collective_id=0, has_side_effects=True, vmem_limit_bytes=67043328),
    )(tokens, routes, routes.T, gates, weights)
    return mixed


def solution(mesh):
    if mesh.shape["exp"] != SIDE * SIDE or mesh.shape["seq"] != 2 * DEPTH:
        raise ValueError("mesh")
    return jax.shard_map(
        body,
        mesh=mesh,
        in_specs=(
            P(("seq", "exp"), None),
            P(("seq", "exp"), None),
            P(("seq", "exp"), None),
            P("exp", "seq", None),
        ),
        out_specs=P(("seq", "exp"), None),
        check_vma=False,
    )
```

```python
import functools

import jax
import jax.numpy as jnp
from jax import lax
from jax.experimental import pallas as pl
from jax.experimental.pallas import tpu as pltpu
from jax.sharding import PartitionSpec as P

SIDE = 4
DEPTH = 4
GROUP = 4
TILE = 8
SENDS = [("b", 2), ("d", 2), ("b", 1), ("d", 1), ("b", 3), ("d", 3), ("b", 0), ("d", 0),
         ("a", 2), ("c", 2), ("a", 1), ("c", 1), ("a", 3), ("c", 3), ("a", 0), ("c", 0)]
SLOTS = [("a", 0), ("b", 0), ("a", 2), ("a", 1), ("a", 3), ("b", 2), ("b", 1), ("b", 3),
         ("c", 0), ("d", 0), ("c", 2), ("c", 1), ("c", 3), ("d", 2), ("d", 1), ("d", 3)]
SELF = [("a", 0), ("c", 0)]
RELAYED = [("b", 2), ("d", 2), ("b", 1), ("d", 1), ("b", 3), ("d", 3)]


def flip(v):
    return v + 1 - 2 * lax.rem(v, 2)


def choose(v, parity, even, odd):
    return even + (odd - even) * lax.rem(parity, 2)


def mate(v, parity):
    return choose(v, parity, flip(v), SIDE - 1 - v)


def beside(v, parity):
    return choose(v, parity, SIDE - 1 - v, flip(v))


def kernel(cap, tok, routes, gates, w, out, held,
           recv, land, rr_lo, rr_hi,
           xsem, wosem, wbsem, tsend, trecv, usend, urecv, lsend, lrecv, hsend, hrecv,
           wloc, wsend, wrecv):
    count, width = tok.shape
    shard, hidden = w.shape[1:]
    rows = 2 * cap
    padded = recv.shape[1]
    sent = -(-rows // TILE) * TILE
    low_rows = cap // 16 * 16
    span = padded - low_rows
    peers = SIDE * SIDE
    experts = 2 * peers
    chunks = 4
    chunk = width // chunks
    f32, bf16 = jnp.float32, jnp.bfloat16

    seq = lax.axis_index("seq")
    exp = lax.axis_index("exp")
    z, core = seq // 2, lax.rem(seq, 2)
    y, x = exp // SIDE, lax.rem(exp, SIDE)
    sibling = 2 * z + 1 - core

    def turn(v, d):
        return lax.rem(v + d + SIDE, SIDE)

    def place(yy, xx):
        return yy * SIDE + xx

    def goal(m):
        kind, d = m
        if kind == "a":
            yy, xx = turn(y, d), x
        elif kind == "b":
            yy = turn(y, d)
            xx = beside(x, yy)
        elif kind == "c":
            yy, xx = y, turn(x, d)
        else:
            xx = turn(x, d)
            yy = beside(y, xx)
        if kind in "ab":
            return (yy, xx), (yy, mate(xx, yy)), 0
        return (yy, xx), (mate(yy, xx), xx), 1

    def corner(m):
        kind, d = m
        if kind == "b":
            return place(y, beside(x, turn(y, d)))
        if kind == "d":
            return place(beside(y, turn(x, d)), x)
        return place(*goal(m)[0])

    def origin(m):
        kind, d = m
        if kind == "a":
            return place(turn(y, -d), x)
        if kind == "b":
            return place(turn(y, -d), beside(x, y))
        if kind == "c":
            return place(y, turn(x, -d))
        return place(beside(y, x), turn(x, -d))

    def names_of(m):
        first, second, which = goal(m)
        return 2 * place(*first) + which, 2 * place(*second) + which

    def rows_of(zz, cc):
        return pl.ds(pl.multiple_of((2 * zz + cc) * shard, shard), shard)

    local_w = pltpu.make_async_copy(w, held.at[pl.ds(0, 2), rows_of(z, core), :], wloc)
    local_w.start()

    barrier = pltpu.get_barrier_semaphore()
    for i in range(1, peers):
        pl.semaphore_signal(barrier, inc=1, device_id={"exp": lax.rem(exp + i, peers)})
    up, down = 2 * lax.rem(z + 1, DEPTH) + core, 2 * lax.rem(z + DEPTH - 1, DEPTH) + core
    for other in (up, down, sibling):
        pl.semaphore_signal(barrier, inc=1, device_id={"seq": other})

    ra, rb = routes[0:1, :], routes[1:2, :]
    names = lax.broadcasted_iota(jnp.int32, (experts, count), 0)
    hit_a, hit_b = names == ra, names == rb
    both = jnp.where(hit_a | hit_b, 1.0, 0.0).astype(bf16)
    earlier = jnp.where(
        lax.broadcasted_iota(jnp.int32, (count, count), 0)
        < lax.broadcasted_iota(jnp.int32, (count, count), 1), 1.0, 0.0).astype(bf16)
    table = (jnp.dot(both, earlier, preferred_element_type=f32)
             + (names * cap).astype(f32))
    pos_a = jnp.sum(jnp.where(hit_a, table, 0.0), axis=0, keepdims=True)
    pos_b = jnp.sum(jnp.where(hit_b, table, 0.0), axis=0, keepdims=True)

    pl.semaphore_wait(barrier, peers - 1 + 3)

    prev, after, far = turn(z, -1), turn(z, 1), turn(z, 2)

    def w_copy(n, part, zz, cc, expert, many, target, mine=False):
        dst = held.at[pl.ds(expert, many), rows_of(zz, cc), :]
        return pltpu.make_async_remote_copy(
            src_ref=w if mine else dst, dst_ref=dst,
            send_sem=wsend.at[10 * part + n], recv_sem=wrecv.at[10 * part + n],
            device_id={"seq": target})

    def swap(j):
        target = place(y, mate(x, y)) if j == 0 else place(mate(y, x), x)
        return pltpu.make_async_remote_copy(
            src_ref=w.at[pl.ds(j, 1)], dst_ref=held.at[pl.ds(2 + j, 1), rows_of(z, core), :],
            send_sem=wsend.at[20 + j], recv_sem=wrecv.at[20 + j], device_id={"exp": target})

    def w_up(p):
        return w_copy(0, p, z, core, 2 * p, 2, up, mine=p == 0)

    def w_down(p):
        return w_copy(1, p, z, core, 2 * p, 2, down, mine=p == 0)

    def w_up_far(p):
        return w_copy(2, p, prev, core, 2 * p, 1, up)

    def w_down_far(p):
        return w_copy(3, p, after, core, 2 * p + 1, 1, down)

    def w_side(p, n, cc):
        zz, expert, many = [(z, 2 * p, 2), (prev, 2 * p, 2), (after, 2 * p, 2),
                            (far, 2 * p, 1), (far, 2 * p + 1, 1)][n]
        return w_copy(4 + n, p, zz, cc, expert, many, sibling, mine=(p == 0 and n == 0 and cc is core))

    def got(copy_n, p):
        zz, expert, many = [(prev, 2 * p, 2), (after, 2 * p, 2), (far, 2 * p, 1), (far, 2 * p + 1, 1)][copy_n]
        w_copy(copy_n, p, zz, core, expert, many, up).wait_recv()

    w_up(0).start()
    w_down(0).start()
    swap(0).start()
    swap(1).start()
    w_side(0, 0, core).start()

    def t_copy(send, m, c):
        i = SENDS.index(m)
        cols = pl.ds(0, width) if c is None else pl.ds(c * chunk, chunk)
        if m in RELAYED:
            dst = land.at[RELAYED.index(m), pl.ds(0, sent), cols]
        else:
            dst = recv.at[SLOTS.index(m), pl.ds(0, sent), cols]
        k = 0 if c is None else c
        return pltpu.make_async_remote_copy(
            src_ref=send.at[i, pl.ds(0, sent), cols], dst_ref=dst,
            send_sem=tsend.at[i, k], recv_sem=trecv.at[i, k], device_id={"exp": corner(m)})

    def pieces(m):
        return range(chunks) if SENDS.index(m) < GROUP else [None]

    def u_copy(m):
        kind, d = m
        target = place(turn(y, d), x) if kind == "b" else place(y, turn(x, d))
        i = RELAYED.index(m)
        return pltpu.make_async_remote_copy(
            src_ref=land.at[i, pl.ds(0, sent), :],
            dst_ref=recv.at[SLOTS.index(m), pl.ds(0, sent), :],
            send_sem=usend.at[i], recv_sem=urecv.at[i], device_id={"exp": target})

    def dispatch(send, xbuf, oh):
        def x_copy(c):
            return pltpu.make_async_copy(
                tok.at[:, pl.ds(c * chunk, chunk)], xbuf.at[c % 2], xsem.at[c % 2])

        x_copy(0).start()
        x_copy(1).start()

        def place_rows(g):
            for i in range(g * GROUP, (g + 1) * GROUP):
                e1, e2 = names_of(SENDS[i])
                r = lax.broadcasted_iota(jnp.int32, (padded, count), 0)
                target = jnp.where(r < cap, r + e1 * cap, r - cap + e2 * cap)
                target = jnp.where(r < rows, target, -1).astype(f32)
                hit = (pos_a == target) | (pos_b == target)
                oh[i * padded:(i + 1) * padded, :] = jnp.where(hit, 1.0, 0.0).astype(bf16)

        groups = peers // GROUP
        for c in range(chunks):
            x_copy(c).wait()
            cols = slice(c * chunk, (c + 1) * chunk)
            for g in range(groups):
                if c == 0:
                    place_rows(g)
                got_rows = jnp.dot(oh[g * GROUP * padded:(g + 1) * GROUP * padded, :], xbuf[c % 2],
                                   preferred_element_type=f32).astype(bf16)
                got_rows = got_rows.reshape(GROUP, padded, chunk)
                ms = SENDS[g * GROUP:(g + 1) * GROUP]
                if g < groups - 1:
                    send[g * GROUP:(g + 1) * GROUP, :, cols] = got_rows
                else:
                    for j, m in enumerate(ms):
                        if m in SELF:
                            recv[SLOTS.index(m), :, cols] = got_rows[j]
                        else:
                            send[g * GROUP + j, :, cols] = got_rows[j]
                for m in ms:
                    if m in SELF:
                        continue
                    if g == 0:
                        t_copy(send, m, c).start()
                    elif c == chunks - 1:
                        t_copy(send, m, None).start()
            if c + 2 < chunks:
                x_copy(c + 2).start()

        def landed(m):
            for c in pieces(m):
                t_copy(send, m, c).wait_recv()

        def relay(m):
            landed(m)
            u_copy(m).start()

        swap(0).wait_recv()
        swap(1).wait_recv()
        w_up(1).start()
        w_down(1).start()
        w_side(1, 0, core).start()
        for m in RELAYED[:4]:
            relay(m)
        local_w.wait()
        got(0, 0)
        w_up_far(0).start()
        w_side(0, 1, core).start()
        got(1, 0)
        w_down_far(0).start()
        w_side(0, 2, core).start()
        for m in RELAYED[4:]:
            relay(m)
        got(0, 1)
        w_up_far(1).start()
        w_side(1, 1, core).start()
        got(1, 1)
        w_down_far(1).start()
        w_side(1, 2, core).start()

        got(2, 0)
        w_side(0, 3, core).start()
        got(3, 0)
        w_side(0, 4, core).start()
        for n in range(5):
            w_side(0, n, 1 - core).wait_recv()

        for m in SENDS:
            if m not in SELF:
                for c in pieces(m):
                    t_copy(send, m, c).wait_send()

    pl.run_scoped(
        dispatch,
        pltpu.VMEM((peers - 2, padded, width), bf16),
        pltpu.VMEM((2, count, chunk), bf16),
        pltpu.VMEM((peers * padded, count), bf16))

    def finish(wown, wbuf, res, acc, pos):
        flat = jnp.concatenate(
            [pos_a, pos_b, gates[0:1, :], gates[1:2, :], jnp.zeros((124, count), f32)], axis=0)
        pos[...] = flat.T

        step = hidden // 2

        def w_load(q, n, slot):
            cols = pl.ds(n * step, step)
            return pltpu.make_async_copy(held.at[q, :, cols], wbuf.at[slot], wbsem.at[slot])

        def own_load(q):
            return pltpu.make_async_copy(held.at[q], wown.at[q], wosem.at[q])

        def own_product(base, q):
            def one(n, carry):
                cols = pl.ds(pl.multiple_of(n * step, step), step)
                left = recv[base:base + GROUP, 0:span, :].reshape(GROUP * span, width)
                prod = jnp.dot(left, wown[q, :, cols], preferred_element_type=f32).astype(bf16)
                res[base:base + GROUP, 0:span, cols] = prod.reshape(GROUP, span, step)
                return carry

            lax.fori_loop(0, hidden // step, one, 0)

        def partner_product(base, n):
            many = 2 * GROUP
            cols = slice(n * step, (n + 1) * step)
            left = recv[base:base + many, low_rows:padded, :].reshape(many * span, width)
            prod = jnp.dot(left, wbuf[n], preferred_element_type=f32).astype(bf16)
            prod = prod.reshape(many, span, step)
            edge = res[base:base + many, low_rows:low_rows + 16, cols]
            r = lax.broadcasted_iota(jnp.int32, edge.shape, 1)
            res[base:base + many, low_rows:low_rows + 16, cols] = jnp.where(
                r < cap - low_rows, edge, prod[:, 0:16])
            res[base:base + many, low_rows + 16:padded, cols] = prod[:, 16:]

        def low_copy(m):
            i = SLOTS.index(m)
            return pltpu.make_async_remote_copy(
                src_ref=res.at[i, pl.ds(0, low_rows), :], dst_ref=rr_lo.at[i],
                send_sem=lsend.at[i], recv_sem=lrecv.at[i], device_id={"exp": origin(m)})

        def high_copy(m):
            i = SLOTS.index(m)
            return pltpu.make_async_remote_copy(
                src_ref=res.at[i, pl.ds(low_rows, sent - low_rows), :],
                dst_ref=rr_hi.at[i, pl.ds(0, sent - low_rows), :],
                send_sem=hsend.at[i], recv_sem=hrecv.at[i], device_id={"exp": origin(m)})

        def arrived(m):
            if m in SELF:
                return
            if m in RELAYED:
                u_copy(m).wait_recv()
            else:
                for c in pieces(m):
                    t_copy(recv, m, c).wait_recv()

        def give_low(base):
            for i in range(base, base + GROUP):
                if SLOTS[i] in SELF:
                    rr_lo[i] = res[i, 0:low_rows, :]
                else:
                    low_copy(SLOTS[i]).start()

        def give_high(base):
            for i in range(base, base + 2 * GROUP):
                if SLOTS[i] in SELF:
                    rr_hi[i] = res[i, low_rows:padded, :]
                else:
                    high_copy(SLOTS[i]).start()

        def all_arrived(base):
            for m in SLOTS[base:base + GROUP]:
                arrived(m)

        own_load(0).start()
        own_load(1).start()
        for base, q in ((0, 0), (8, 1)):
            all_arrived(base)
            own_load(q).wait()
            own_product(base, q)
            give_low(base)

        for base, q in ((4, 0), (12, 1)):
            all_arrived(base)
            own_product(base, q)
            give_low(base)

        got(2, 1)
        w_side(1, 3, core).start()
        got(3, 1)
        w_side(1, 4, core).start()
        for n in range(5):
            w_side(1, n, 1 - core).wait_recv()

        for n in range(2):
            w_load(2, n, n).start()
        for base, q in ((0, 2), (8, 3)):
            for n in range(2):
                w_load(q, n, n).wait()
                partner_product(base, n)
                if q == 2:
                    w_load(3, n, n).start()
            give_high(base)

        slot_a, slot_b = pos[:, 0:1], pos[:, 1:2]
        gate_a, gate_b = pos[:, 2:3], pos[:, 3:4]

        def mixed(base, high):
            size = span if high else low_rows
            lane = lax.broadcasted_iota(jnp.int32, (1, GROUP * size), 1)
            target = jnp.full_like(lane, -1)
            for j in range(GROUP):
                e1, e2 = names_of(SLOTS[base + j])
                local = lane - j * size
                r = local + (low_rows if high else 0)
                value = jnp.where(r < cap, r + e1 * cap, r - cap + e2 * cap)
                target = jnp.where((local >= 0) & (local < size) & (r < rows), value, target)
            target = target.astype(f32)
            mix = jnp.where(slot_a == target, gate_a, 0.0) + jnp.where(slot_b == target, gate_b, 0.0)
            top = mix.astype(bf16)
            rest = (mix - top.astype(f32)).astype(bf16)
            for m in SLOTS[base:base + GROUP]:
                if m not in SELF:
                    (high_copy(m) if high else low_copy(m)).wait_recv()
            if high:
                right = rr_hi[base:base + GROUP]
                r = lax.broadcasted_iota(jnp.int32, right.shape, 1)
                right = jnp.where(r < rows - low_rows, right, jnp.zeros_like(right))
            else:
                right = rr_lo[base:base + GROUP]
            right = right.reshape(GROUP * size, hidden)
            return (jnp.dot(top, right, preferred_element_type=f32)
                    + jnp.dot(rest, right, preferred_element_type=f32))

        order = [(0, False), (8, False), (4, False), (12, False),
                 (0, True), (8, True), (4, True), (12, True)]
        for k, (base, high) in enumerate(order):
            part = mixed(base, high)
            if k == 0:
                acc[...] = part
            elif k < len(order) - 1:
                acc[...] += part
            else:
                out[...] = (acc[...] + part).astype(bf16)

        for m in SENDS:
            if m not in SELF:
                low_copy(m).wait_send()
                high_copy(m).wait_send()

    pl.run_scoped(
        finish,
        pltpu.VMEM((2, width, hidden), bf16),
        pltpu.VMEM((2, width, hidden // 2), bf16),
        pltpu.VMEM((peers, padded, hidden), bf16),
        pltpu.VMEM((count, hidden), f32),
        pltpu.VMEM((count, 128), f32))

    for m in RELAYED:
        u_copy(m).wait_send()
    swap(0).wait_send()
    swap(1).wait_send()
    for p in range(2):
        for copy in (w_up(p), w_down(p), w_up_far(p), w_down_far(p)):
            copy.wait_send()
        for n in range(5):
            w_side(p, n, core).wait_send()


def body(tokens, routes, gates, weights):
    peers = SIDE * SIDE
    count, width = tokens.shape
    shard, hidden = weights.shape[1:]
    cap = 5 * count // (4 * peers)
    rows = 2 * cap
    padded = -(-rows // 16) * 16
    low_rows = cap // 16 * 16
    span = padded - low_rows
    bf16 = jnp.bfloat16
    dma = pltpu.SemaphoreType.DMA
    vmem = pl.BlockSpec(memory_space=pltpu.VMEM)
    anywhere = pl.BlockSpec(memory_space=pl.ANY)
    mixed, _ = pl.pallas_call(
        functools.partial(kernel, cap),
        out_shape=(
            jax.ShapeDtypeStruct((count, hidden), bf16),
            jax.ShapeDtypeStruct((4, width, hidden), bf16),
        ),
        in_specs=[anywhere, vmem, vmem, anywhere],
        out_specs=(vmem, anywhere),
        scratch_shapes=[
            pltpu.VMEM((peers, padded, width), bf16),
            pltpu.VMEM((len(RELAYED), padded, width), bf16),
            pltpu.VMEM((peers, low_rows, hidden), bf16),
            pltpu.VMEM((peers, span, hidden), bf16),
            dma((2,)),
            dma((2,)),
            dma((2,)),
            dma((peers, 4)),
            dma((peers, 4)),
            dma((len(RELAYED),)),
            dma((len(RELAYED),)),
            dma((peers,)),
            dma((peers,)),
            dma((peers,)),
            dma((peers,)),
            dma,
            dma((22,)),
            dma((22,)),
        ],
        compiler_params=pltpu.CompilerParams(
            collective_id=0, has_side_effects=True, vmem_limit_bytes=67043328),
    )(tokens, routes.T, gates.T, weights)
    return mixed


def solution(mesh):
    if mesh.shape["exp"] != SIDE * SIDE or mesh.shape["seq"] != 2 * DEPTH:
        raise ValueError("mesh")
    return jax.shard_map(
        body,
        mesh=mesh,
        in_specs=(
            P(("seq", "exp"), None),
            P(("seq", "exp"), None),
            P(("seq", "exp"), None),
            P("exp", "seq", None),
        ),
        out_specs=P(("seq", "exp"), None),
        check_vma=False,
    )
```

```python
import functools

import jax
import jax.numpy as jnp
from jax import lax
from jax.experimental import pallas as pl
from jax.experimental.pallas import tpu as pltpu
from jax.sharding import PartitionSpec as P

SIDE = 4
DEPTH = 4
GROUP = 4
TILE = 8
SENDS = [("b", 2), ("d", 2), ("b", 1), ("d", 1), ("b", 3), ("d", 3), ("b", 0), ("d", 0),
         ("a", 2), ("c", 2), ("a", 1), ("c", 1), ("a", 3), ("c", 3), ("a", 0), ("c", 0)]
SLOTS = [("a", 0), ("b", 0), ("a", 2), ("a", 1), ("a", 3), ("b", 2), ("b", 1), ("b", 3),
         ("c", 0), ("d", 0), ("c", 2), ("c", 1), ("c", 3), ("d", 2), ("d", 1), ("d", 3)]
SELF = [("a", 0), ("c", 0)]
RING_FIRST = [("b", 1), ("d", 1)]
RELAYED = [("b", 2), ("d", 2), ("b", 1), ("d", 1), ("b", 3), ("d", 3)]


def flip(v):
    return v + 1 - 2 * lax.rem(v, 2)


def choose(v, parity, even, odd):
    return even + (odd - even) * lax.rem(parity, 2)


def mate(v, parity):
    return choose(v, parity, flip(v), SIDE - 1 - v)


def beside(v, parity):
    return choose(v, parity, SIDE - 1 - v, flip(v))


def kernel(cap, tok, routes, gates, w, out, held,
           recv, land, rr_lo, rr_hi,
           xsem, wosem, wbsem, tsend, trecv, usend, urecv, lsend, lrecv, hsend, hrecv,
           wloc, wsend, wrecv):
    count, width = tok.shape
    shard, hidden = w.shape[1:]
    rows = 2 * cap
    padded = recv.shape[1]
    sent = -(-rows // TILE) * TILE
    low_rows = cap // 16 * 16
    span = padded - low_rows
    peers = SIDE * SIDE
    experts = 2 * peers
    chunks = 4
    chunk = width // chunks
    f32, bf16 = jnp.float32, jnp.bfloat16

    seq = lax.axis_index("seq")
    exp = lax.axis_index("exp")
    z, core = seq // 2, lax.rem(seq, 2)
    y, x = exp // SIDE, lax.rem(exp, SIDE)
    sibling = 2 * z + 1 - core

    def turn(v, d):
        return lax.rem(v + d + SIDE, SIDE)

    def place(yy, xx):
        return yy * SIDE + xx

    def goal(m):
        kind, d = m
        if kind == "a":
            yy, xx = turn(y, d), x
        elif kind == "b":
            yy = turn(y, d)
            xx = beside(x, yy)
        elif kind == "c":
            yy, xx = y, turn(x, d)
        else:
            xx = turn(x, d)
            yy = beside(y, xx)
        if kind in "ab":
            return (yy, xx), (yy, mate(xx, yy)), 0
        return (yy, xx), (mate(yy, xx), xx), 1

    def corner(m):
        kind, d = m
        if m in RING_FIRST:
            return place(turn(y, d), x) if kind == "b" else place(y, turn(x, d))
        if kind == "b":
            return place(y, beside(x, turn(y, d)))
        if kind == "d":
            return place(beside(y, turn(x, d)), x)
        return place(*goal(m)[0])

    def origin(m):
        kind, d = m
        if kind == "a":
            return place(turn(y, -d), x)
        if kind == "b":
            return place(turn(y, -d), beside(x, y))
        if kind == "c":
            return place(y, turn(x, -d))
        return place(beside(y, x), turn(x, -d))

    def names_of(m):
        first, second, which = goal(m)
        return 2 * place(*first) + which, 2 * place(*second) + which

    def rows_of(zz, cc):
        return pl.ds(pl.multiple_of((2 * zz + cc) * shard, shard), shard)

    local_w = pltpu.make_async_copy(w, held.at[pl.ds(0, 2), rows_of(z, core), :], wloc)
    local_w.start()

    barrier = pltpu.get_barrier_semaphore()
    for i in range(1, peers):
        pl.semaphore_signal(barrier, inc=1, device_id={"exp": lax.rem(exp + i, peers)})
    up, down = 2 * lax.rem(z + 1, DEPTH) + core, 2 * lax.rem(z + DEPTH - 1, DEPTH) + core
    for other in (up, down, sibling):
        pl.semaphore_signal(barrier, inc=1, device_id={"seq": other})

    ra, rb = routes[0:1, :], routes[1:2, :]
    names = lax.broadcasted_iota(jnp.int32, (experts, count), 0)
    hit_a, hit_b = names == ra, names == rb
    both = jnp.where(hit_a | hit_b, 1.0, 0.0).astype(bf16)
    earlier = jnp.where(
        lax.broadcasted_iota(jnp.int32, (count, count), 0)
        < lax.broadcasted_iota(jnp.int32, (count, count), 1), 1.0, 0.0).astype(bf16)
    table = (jnp.dot(both, earlier, preferred_element_type=f32)
             + (names * cap).astype(f32))
    pos_a = jnp.sum(jnp.where(hit_a, table, 0.0), axis=0, keepdims=True)
    pos_b = jnp.sum(jnp.where(hit_b, table, 0.0), axis=0, keepdims=True)

    pl.semaphore_wait(barrier, peers - 1 + 3)

    prev, after, far = turn(z, -1), turn(z, 1), turn(z, 2)

    def w_copy(n, part, zz, cc, expert, many, target, mine=False, half=None):
        if half is None:
            row = rows_of(zz, cc)
        else:
            row = pl.ds(pl.multiple_of((2 * zz + cc) * shard + half * (shard // 2), shard // 2), shard // 2)
        dst = held.at[pl.ds(expert, many), row, :]
        return pltpu.make_async_remote_copy(
            src_ref=w if mine else dst, dst_ref=dst,
            send_sem=wsend.at[10 * part + n], recv_sem=wrecv.at[10 * part + n],
            device_id={"seq": target})

    def swap(j):
        target = place(y, mate(x, y)) if j == 0 else place(mate(y, x), x)
        return pltpu.make_async_remote_copy(
            src_ref=w.at[pl.ds(j, 1)], dst_ref=held.at[pl.ds(2 + j, 1), rows_of(z, core), :],
            send_sem=wsend.at[30 + j], recv_sem=wrecv.at[30 + j], device_id={"exp": target})

    def whole(p):
        return (0, 2) if p == 0 else (1 + p, 1)

    def part_of(p, side):
        return (side, 1, None) if p == 0 else (1 + p, 1, side)

    def w_up(p):
        return w_copy(0, p, z, core, *whole(p), up, mine=p == 0)

    def w_down(p):
        return w_copy(1, p, z, core, *whole(p), down, mine=p == 0)

    def w_up_far(p):
        expert, many, half = part_of(p, 0)
        return w_copy(2, p, prev, core, expert, many, up, half=half)

    def w_down_far(p):
        expert, many, half = part_of(p, 1)
        return w_copy(3, p, after, core, expert, many, down, half=half)

    def w_side(p, n, cc):
        zz = (z, prev, after, far, far)[n]
        expert, many, half = (*whole(p), None) if n < 3 else part_of(p, n - 3)
        return w_copy(4 + n, p, zz, cc, expert, many, sibling,
                      mine=(p == 0 and n == 0 and cc is core), half=half)

    def got(n, p):
        zz = (prev, after, far, far)[n]
        expert, many, half = (*whole(p), None) if n < 2 else part_of(p, n - 2)
        w_copy(n, p, zz, core, expert, many, up, half=half).wait_recv()

    w_up(0).start()
    w_down(0).start()
    swap(0).start()
    swap(1).start()
    w_side(0, 0, core).start()

    def t_copy(send, m, c):
        i = SENDS.index(m)
        cols = pl.ds(0, width) if c is None else pl.ds(c * chunk, chunk)
        if m in RELAYED:
            dst = land.at[RELAYED.index(m), pl.ds(0, sent), cols]
        else:
            dst = recv.at[SLOTS.index(m), pl.ds(0, sent), cols]
        k = 0 if c is None else c
        return pltpu.make_async_remote_copy(
            src_ref=send.at[i, pl.ds(0, sent), cols], dst_ref=dst,
            send_sem=tsend.at[i, k], recv_sem=trecv.at[i, k], device_id={"exp": corner(m)})

    def pieces(m):
        return range(chunks) if SENDS.index(m) < GROUP else [None]

    def u_copy(m):
        kind, d = m
        if m in RING_FIRST:
            target = place(y, beside(x, y)) if kind == "b" else place(beside(y, x), x)
        else:
            target = place(turn(y, d), x) if kind == "b" else place(y, turn(x, d))
        i = RELAYED.index(m)
        return pltpu.make_async_remote_copy(
            src_ref=land.at[i, pl.ds(0, sent), :],
            dst_ref=recv.at[SLOTS.index(m), pl.ds(0, sent), :],
            send_sem=usend.at[i], recv_sem=urecv.at[i], device_id={"exp": target})

    def dispatch(send, xbuf, oh):
        def x_copy(c):
            return pltpu.make_async_copy(
                tok.at[:, pl.ds(c * chunk, chunk)], xbuf.at[c % 2], xsem.at[c % 2])

        x_copy(0).start()
        x_copy(1).start()

        def place_rows(g):
            for i in range(g * GROUP, (g + 1) * GROUP):
                e1, e2 = names_of(SENDS[i])
                r = lax.broadcasted_iota(jnp.int32, (padded, count), 0)
                target = jnp.where(r < cap, r + e1 * cap, r - cap + e2 * cap)
                target = jnp.where(r < rows, target, -1).astype(f32)
                hit = (pos_a == target) | (pos_b == target)
                oh[i * padded:(i + 1) * padded, :] = jnp.where(hit, 1.0, 0.0).astype(bf16)

        groups = peers // GROUP
        for c in range(chunks):
            x_copy(c).wait()
            cols = slice(c * chunk, (c + 1) * chunk)
            for g in range(groups):
                if c == 0:
                    place_rows(g)
                got_rows = jnp.dot(oh[g * GROUP * padded:(g + 1) * GROUP * padded, :], xbuf[c % 2],
                                   preferred_element_type=f32).astype(bf16)
                got_rows = got_rows.reshape(GROUP, padded, chunk)
                ms = SENDS[g * GROUP:(g + 1) * GROUP]
                if g < groups - 1:
                    send[g * GROUP:(g + 1) * GROUP, :, cols] = got_rows
                else:
                    for j, m in enumerate(ms):
                        if m in SELF:
                            recv[SLOTS.index(m), :, cols] = got_rows[j]
                        else:
                            send[g * GROUP + j, :, cols] = got_rows[j]
                for m in ms:
                    if m in SELF:
                        continue
                    if g == 0:
                        t_copy(send, m, c).start()
                    elif c == chunks - 1:
                        t_copy(send, m, None).start()
            if c + 2 < chunks:
                x_copy(c + 2).start()

        def landed(m):
            for c in pieces(m):
                t_copy(send, m, c).wait_recv()

        def relay(m):
            landed(m)
            u_copy(m).start()

        for j in range(2):
            swap(j).wait_recv()
            w_up(1 + j).start()
            w_down(1 + j).start()
            w_side(1 + j, 0, core).start()
        for m in RELAYED[:4]:
            relay(m)
        local_w.wait()
        got(0, 0)
        w_up_far(0).start()
        w_side(0, 1, core).start()
        got(1, 0)
        w_down_far(0).start()
        w_side(0, 2, core).start()
        for m in RELAYED[4:]:
            relay(m)
        for p in (1, 2):
            got(0, p)
            w_up_far(p).start()
            w_side(p, 1, core).start()
            got(1, p)
            w_down_far(p).start()
            w_side(p, 2, core).start()

        got(2, 0)
        w_side(0, 3, core).start()
        got(3, 0)
        w_side(0, 4, core).start()
        for n in range(5):
            w_side(0, n, 1 - core).wait_recv()

        for m in SENDS:
            if m not in SELF:
                for c in pieces(m):
                    t_copy(send, m, c).wait_send()

    pl.run_scoped(
        dispatch,
        pltpu.VMEM((peers - 2, padded, width), bf16),
        pltpu.VMEM((2, count, chunk), bf16),
        pltpu.VMEM((peers * padded, count), bf16))

    def finish(wown, wbuf, res, acc, pos):
        flat = jnp.concatenate(
            [pos_a, pos_b, gates[0:1, :], gates[1:2, :], jnp.zeros((124, count), f32)], axis=0)
        pos[...] = flat.T

        step = hidden // 2

        def w_load(q, n, slot):
            cols = pl.ds(n * step, step)
            return pltpu.make_async_copy(held.at[q, :, cols], wbuf.at[slot], wbsem.at[slot])

        def own_load(q):
            return pltpu.make_async_copy(held.at[q], wown.at[q], wosem.at[q])

        def own_product(base, q):
            def one(n, carry):
                cols = pl.ds(pl.multiple_of(n * step, step), step)
                left = recv[base:base + GROUP, 0:span, :].reshape(GROUP * span, width)
                prod = jnp.dot(left, wown[q, :, cols], preferred_element_type=f32).astype(bf16)
                res[base:base + GROUP, 0:span, cols] = prod.reshape(GROUP, span, step)
                return carry

            lax.fori_loop(0, hidden // step, one, 0)

        def partner_product(base, n):
            many = 2 * GROUP
            cols = slice(n * step, (n + 1) * step)
            left = recv[base:base + many, low_rows:padded, :].reshape(many * span, width)
            prod = jnp.dot(left, wbuf[n], preferred_element_type=f32).astype(bf16)
            prod = prod.reshape(many, span, step)
            edge = res[base:base + many, low_rows:low_rows + 16, cols]
            r = lax.broadcasted_iota(jnp.int32, edge.shape, 1)
            res[base:base + many, low_rows:low_rows + 16, cols] = jnp.where(
                r < cap - low_rows, edge, prod[:, 0:16])
            res[base:base + many, low_rows + 16:padded, cols] = prod[:, 16:]

        def low_copy(m):
            i = SLOTS.index(m)
            return pltpu.make_async_remote_copy(
                src_ref=res.at[i, pl.ds(0, low_rows), :], dst_ref=rr_lo.at[i],
                send_sem=lsend.at[i], recv_sem=lrecv.at[i], device_id={"exp": origin(m)})

        def high_copy(m, n):
            i = SLOTS.index(m)
            cols = pl.ds(n * step, step)
            return pltpu.make_async_remote_copy(
                src_ref=res.at[i, pl.ds(low_rows, sent - low_rows), cols],
                dst_ref=rr_hi.at[i, pl.ds(0, sent - low_rows), cols],
                send_sem=hsend.at[i, n], recv_sem=hrecv.at[i, n], device_id={"exp": origin(m)})

        def arrived(m):
            if m in SELF:
                return
            if m in RELAYED:
                u_copy(m).wait_recv()
            else:
                for c in pieces(m):
                    t_copy(recv, m, c).wait_recv()

        def give_low(base):
            for i in reversed(range(base, base + GROUP)):
                if SLOTS[i] in SELF:
                    rr_lo[i] = res[i, 0:low_rows, :]
                else:
                    low_copy(SLOTS[i]).start()

        def give_high(base, n):
            for i in reversed(range(base, base + 2 * GROUP)):
                if SLOTS[i] in SELF:
                    cols = slice(n * step, (n + 1) * step)
                    rr_hi[i, :, cols] = res[i, low_rows:padded, cols]
                else:
                    high_copy(SLOTS[i], n).start()

        def all_arrived(base):
            for m in SLOTS[base:base + GROUP]:
                arrived(m)

        own_load(0).start()
        own_load(1).start()
        for base, q in ((0, 0), (8, 1)):
            all_arrived(base)
            own_load(q).wait()
            own_product(base, q)
            give_low(base)

        for base, q in ((4, 0), (12, 1)):
            all_arrived(base)
            own_product(base, q)
            give_low(base)

        def far_part(p):
            got(2, p)
            w_side(p, 3, core).start()
            got(3, p)
            w_side(p, 4, core).start()

        def complete(p):
            for n in range(5):
                w_side(p, n, 1 - core).wait_recv()
            for n in range(2):
                w_load(1 + p, n, n).start()

        far_part(1)
        complete(1)
        for n in range(2):
            w_load(2, n, n).wait()
            partner_product(0, n)
            give_high(0, n)
            if n == 0:
                far_part(2)
        complete(2)
        for n in range(2):
            w_load(3, n, n).wait()
            partner_product(8, n)
            give_high(8, n)

        slot_a, slot_b = pos[:, 0:1], pos[:, 1:2]
        gate_a, gate_b = pos[:, 2:3], pos[:, 3:4]

        def mixed(base, high):
            size = span if high else low_rows
            lane = lax.broadcasted_iota(jnp.int32, (1, GROUP * size), 1)
            target = jnp.full_like(lane, -1)
            for j in range(GROUP):
                e1, e2 = names_of(SLOTS[base + j])
                local = lane - j * size
                r = local + (low_rows if high else 0)
                value = jnp.where(r < cap, r + e1 * cap, r - cap + e2 * cap)
                target = jnp.where((local >= 0) & (local < size) & (r < rows), value, target)
            target = target.astype(f32)
            mix = jnp.where(slot_a == target, gate_a, 0.0) + jnp.where(slot_b == target, gate_b, 0.0)
            top = mix.astype(bf16)
            rest = (mix - top.astype(f32)).astype(bf16)
            for m in SLOTS[base:base + GROUP]:
                if m not in SELF:
                    for copy in ([high_copy(m, n) for n in range(2)] if high else [low_copy(m)]):
                        copy.wait_recv()
            if high:
                right = rr_hi[base:base + GROUP]
                r = lax.broadcasted_iota(jnp.int32, right.shape, 1)
                right = jnp.where(r < rows - low_rows, right, jnp.zeros_like(right))
            else:
                right = rr_lo[base:base + GROUP]
            right = right.reshape(GROUP * size, hidden)
            return (jnp.dot(top, right, preferred_element_type=f32)
                    + jnp.dot(rest, right, preferred_element_type=f32))

        order = [(0, False), (8, False), (4, False), (12, False),
                 (4, True), (0, True), (12, True), (8, True)]
        for k, (base, high) in enumerate(order):
            part = mixed(base, high)
            if k == 0:
                acc[...] = part
            elif k < len(order) - 1:
                acc[...] += part
            else:
                out[...] = (acc[...] + part).astype(bf16)

        for m in SENDS:
            if m not in SELF:
                low_copy(m).wait_send()
                for n in range(2):
                    high_copy(m, n).wait_send()

    pl.run_scoped(
        finish,
        pltpu.VMEM((2, width, hidden), bf16),
        pltpu.VMEM((2, width, hidden // 2), bf16),
        pltpu.VMEM((peers, padded, hidden), bf16),
        pltpu.VMEM((count, hidden), f32),
        pltpu.VMEM((count, 128), f32))

    for m in RELAYED:
        u_copy(m).wait_send()
    swap(0).wait_send()
    swap(1).wait_send()
    for p in range(3):
        for copy in (w_up(p), w_down(p), w_up_far(p), w_down_far(p)):
            copy.wait_send()
        for n in range(5):
            w_side(p, n, core).wait_send()


def body(tokens, routes, gates, weights):
    peers = SIDE * SIDE
    count, width = tokens.shape
    shard, hidden = weights.shape[1:]
    cap = 5 * count // (4 * peers)
    rows = 2 * cap
    padded = -(-rows // 16) * 16
    low_rows = cap // 16 * 16
    span = padded - low_rows
    bf16 = jnp.bfloat16
    dma = pltpu.SemaphoreType.DMA
    vmem = pl.BlockSpec(memory_space=pltpu.VMEM)
    anywhere = pl.BlockSpec(memory_space=pl.ANY)
    mixed, _ = pl.pallas_call(
        functools.partial(kernel, cap),
        out_shape=(
            jax.ShapeDtypeStruct((count, hidden), bf16),
            jax.ShapeDtypeStruct((4, width, hidden), bf16),
        ),
        in_specs=[anywhere, vmem, vmem, anywhere],
        out_specs=(vmem, anywhere),
        scratch_shapes=[
            pltpu.VMEM((peers, padded, width), bf16),
            pltpu.VMEM((len(RELAYED), padded, width), bf16),
            pltpu.VMEM((peers, low_rows, hidden), bf16),
            pltpu.VMEM((peers, span, hidden), bf16),
            dma((2,)),
            dma((2,)),
            dma((2,)),
            dma((peers, 4)),
            dma((peers, 4)),
            dma((len(RELAYED),)),
            dma((len(RELAYED),)),
            dma((peers,)),
            dma((peers,)),
            dma((peers, 2)),
            dma((peers, 2)),
            dma,
            dma((32,)),
            dma((32,)),
        ],
        compiler_params=pltpu.CompilerParams(
            collective_id=0, has_side_effects=True, vmem_limit_bytes=67043328),
    )(tokens, routes.T, gates.T, weights)
    return mixed


def solution(mesh):
    if mesh.shape["exp"] != SIDE * SIDE or mesh.shape["seq"] != 2 * DEPTH:
        raise ValueError("mesh")
    return jax.shard_map(
        body,
        mesh=mesh,
        in_specs=(
            P(("seq", "exp"), None),
            P(("seq", "exp"), None),
            P(("seq", "exp"), None),
            P("exp", "seq", None),
        ),
        out_specs=P(("seq", "exp"), None),
        check_vma=False,
    )
```

```python
import functools

import jax
import jax.numpy as jnp
from jax import lax
from jax.experimental import pallas as pl
from jax.experimental.pallas import tpu as pltpu
from jax.sharding import PartitionSpec as P

SIDE = 4
DEPTH = 4
GROUP = 4
TILE = 8
SENDS = [("b", 2), ("d", 2), ("b", 1), ("d", 1), ("b", 3), ("d", 3), ("b", 0), ("d", 0),
         ("a", 2), ("c", 2), ("a", 1), ("c", 1), ("a", 3), ("c", 3), ("a", 0), ("c", 0)]
SLOTS = [("a", 0), ("b", 0), ("a", 2), ("a", 1), ("a", 3), ("b", 2), ("b", 1), ("b", 3),
         ("c", 0), ("d", 0), ("c", 2), ("c", 1), ("c", 3), ("d", 2), ("d", 1), ("d", 3)]
SELF = [("a", 0), ("c", 0)]
RING_FIRST = [("b", 1), ("d", 1)]
RELAYED = [("b", 2), ("d", 2), ("b", 1), ("d", 1), ("b", 3), ("d", 3)]


def flip(v):
    return v + 1 - 2 * lax.rem(v, 2)


def choose(v, parity, even, odd):
    return even + (odd - even) * lax.rem(parity, 2)


def mate(v, parity):
    return choose(v, parity, flip(v), SIDE - 1 - v)


def beside(v, parity):
    return choose(v, parity, SIDE - 1 - v, flip(v))


def kernel(cap, tok, routes, gates, w, out, held,
           recv, land, rr_lo, rr_hi,
           xsem, wosem, wbsem, tsend, trecv, usend, urecv, lsend, lrecv, hsend, hrecv,
           wloc, wsend, wrecv):
    count, width = tok.shape
    shard, hidden = w.shape[1:]
    rows = 2 * cap
    padded = recv.shape[1]
    sent = -(-rows // TILE) * TILE
    low_rows = cap // 16 * 16
    span = padded - low_rows
    peers = SIDE * SIDE
    experts = 2 * peers
    chunks = 4
    chunk = width // chunks
    f32, bf16 = jnp.float32, jnp.bfloat16

    seq = lax.axis_index("seq")
    exp = lax.axis_index("exp")
    z, core = seq // 2, lax.rem(seq, 2)
    y, x = exp // SIDE, lax.rem(exp, SIDE)
    sibling = 2 * z + 1 - core

    def turn(v, d):
        return lax.rem(v + d + SIDE, SIDE)

    def place(yy, xx):
        return yy * SIDE + xx

    def goal(m):
        kind, d = m
        if kind == "a":
            yy, xx = turn(y, d), x
        elif kind == "b":
            yy = turn(y, d)
            xx = beside(x, yy)
        elif kind == "c":
            yy, xx = y, turn(x, d)
        else:
            xx = turn(x, d)
            yy = beside(y, xx)
        if kind in "ab":
            return (yy, xx), (yy, mate(xx, yy)), 0
        return (yy, xx), (mate(yy, xx), xx), 1

    def corner(m):
        kind, d = m
        if m in RING_FIRST:
            return place(turn(y, d), x) if kind == "b" else place(y, turn(x, d))
        if kind == "b":
            return place(y, beside(x, turn(y, d)))
        if kind == "d":
            return place(beside(y, turn(x, d)), x)
        return place(*goal(m)[0])

    def origin(m):
        kind, d = m
        if kind == "a":
            return place(turn(y, -d), x)
        if kind == "b":
            return place(turn(y, -d), beside(x, y))
        if kind == "c":
            return place(y, turn(x, -d))
        return place(beside(y, x), turn(x, -d))

    def names_of(m):
        first, second, which = goal(m)
        return 2 * place(*first) + which, 2 * place(*second) + which

    def rows_of(zz, cc):
        return pl.ds(pl.multiple_of((2 * zz + cc) * shard, shard), shard)

    local_w = pltpu.make_async_copy(w, held.at[pl.ds(0, 2), rows_of(z, core), :], wloc)
    local_w.start()

    barrier = pltpu.get_barrier_semaphore()
    for i in range(1, peers):
        pl.semaphore_signal(barrier, inc=1, device_id={"exp": lax.rem(exp + i, peers)})
    up, down = 2 * lax.rem(z + 1, DEPTH) + core, 2 * lax.rem(z + DEPTH - 1, DEPTH) + core
    for other in (up, down, sibling):
        pl.semaphore_signal(barrier, inc=1, device_id={"seq": other})

    ra, rb = routes[0:1, :], routes[1:2, :]
    names = lax.broadcasted_iota(jnp.int32, (experts, count), 0)
    hit_a, hit_b = names == ra, names == rb
    both = jnp.where(hit_a | hit_b, 1.0, 0.0).astype(bf16)
    earlier = jnp.where(
        lax.broadcasted_iota(jnp.int32, (count, count), 0)
        < lax.broadcasted_iota(jnp.int32, (count, count), 1), 1.0, 0.0).astype(bf16)
    table = (jnp.dot(both, earlier, preferred_element_type=f32)
             + (names * cap).astype(f32))
    pos_a = jnp.sum(jnp.where(hit_a, table, 0.0), axis=0, keepdims=True)
    pos_b = jnp.sum(jnp.where(hit_b, table, 0.0), axis=0, keepdims=True)

    pl.semaphore_wait(barrier, peers - 1 + 3)

    prev, after, far = turn(z, -1), turn(z, 1), turn(z, 2)

    def w_copy(n, part, zz, cc, expert, many, target, mine=False):
        cols = pl.ds(0, hidden) if part == 0 else pl.ds((part - 1) * (hidden // 2), hidden // 2)
        dst = held.at[pl.ds(expert, many), rows_of(zz, cc), cols]
        return pltpu.make_async_remote_copy(
            src_ref=w if mine else dst, dst_ref=dst,
            send_sem=wsend.at[10 * part + n], recv_sem=wrecv.at[10 * part + n],
            device_id={"seq": target})

    def swap(j):
        target = place(y, mate(x, y)) if j == 0 else place(mate(y, x), x)
        return pltpu.make_async_remote_copy(
            src_ref=w.at[pl.ds(j, 1)], dst_ref=held.at[pl.ds(2 + j, 1), rows_of(z, core), :],
            send_sem=wsend.at[30 + j], recv_sem=wrecv.at[30 + j], device_id={"exp": target})

    def first_of(p):
        return 0 if p == 0 else 2

    def w_up(p):
        return w_copy(0, p, z, core, first_of(p), 2, up, mine=p == 0)

    def w_down(p):
        return w_copy(1, p, z, core, first_of(p), 2, down, mine=p == 0)

    def w_up_far(p):
        return w_copy(2, p, prev, core, first_of(p), 1, up)

    def w_down_far(p):
        return w_copy(3, p, after, core, first_of(p) + 1, 1, down)

    def w_side(p, n, cc):
        zz = (z, prev, after, far, far)[n]
        expert, many = first_of(p) + (n == 4), 2 if n < 3 else 1
        return w_copy(4 + n, p, zz, cc, expert, many, sibling,
                      mine=(p == 0 and n == 0 and cc is core))

    def got(n, p):
        zz = (prev, after, far, far)[n]
        expert, many = first_of(p) + (n == 3), 2 if n < 2 else 1
        w_copy(n, p, zz, core, expert, many, up).wait_recv()

    w_up(0).start()
    w_down(0).start()
    swap(0).start()
    swap(1).start()
    w_side(0, 0, core).start()

    def t_copy(send, m, c):
        i = SENDS.index(m)
        cols = pl.ds(0, width) if c is None else pl.ds(c * chunk, chunk)
        if m in RELAYED:
            dst = land.at[RELAYED.index(m), pl.ds(0, sent), cols]
        else:
            dst = recv.at[SLOTS.index(m), pl.ds(0, sent), cols]
        k = 0 if c is None else c
        return pltpu.make_async_remote_copy(
            src_ref=send.at[i, pl.ds(0, sent), cols], dst_ref=dst,
            send_sem=tsend.at[i, k], recv_sem=trecv.at[i, k], device_id={"exp": corner(m)})

    def pieces(m):
        return range(chunks) if SENDS.index(m) < GROUP else [None]

    def u_copy(m):
        kind, d = m
        if m in RING_FIRST:
            target = place(y, beside(x, y)) if kind == "b" else place(beside(y, x), x)
        else:
            target = place(turn(y, d), x) if kind == "b" else place(y, turn(x, d))
        i = RELAYED.index(m)
        return pltpu.make_async_remote_copy(
            src_ref=land.at[i, pl.ds(0, sent), :],
            dst_ref=recv.at[SLOTS.index(m), pl.ds(0, sent), :],
            send_sem=usend.at[i], recv_sem=urecv.at[i], device_id={"exp": target})

    def dispatch(send, xbuf, oh):
        def x_copy(c):
            return pltpu.make_async_copy(
                tok.at[:, pl.ds(c * chunk, chunk)], xbuf.at[c % 2], xsem.at[c % 2])

        x_copy(0).start()
        x_copy(1).start()

        def place_rows(g):
            for i in range(g * GROUP, (g + 1) * GROUP):
                e1, e2 = names_of(SENDS[i])
                r = lax.broadcasted_iota(jnp.int32, (padded, count), 0)
                target = jnp.where(r < cap, r + e1 * cap, r - cap + e2 * cap)
                target = jnp.where(r < rows, target, -1).astype(f32)
                hit = (pos_a == target) | (pos_b == target)
                oh[i * padded:(i + 1) * padded, :] = jnp.where(hit, 1.0, 0.0).astype(bf16)

        groups = peers // GROUP
        for c in range(chunks):
            x_copy(c).wait()
            cols = slice(c * chunk, (c + 1) * chunk)
            for g in range(groups):
                if c == 0:
                    place_rows(g)
                got_rows = jnp.dot(oh[g * GROUP * padded:(g + 1) * GROUP * padded, :], xbuf[c % 2],
                                   preferred_element_type=f32).astype(bf16)
                got_rows = got_rows.reshape(GROUP, padded, chunk)
                ms = SENDS[g * GROUP:(g + 1) * GROUP]
                if g < groups - 1:
                    send[g * GROUP:(g + 1) * GROUP, :, cols] = got_rows
                else:
                    for j, m in enumerate(ms):
                        if m in SELF:
                            recv[SLOTS.index(m), :, cols] = got_rows[j]
                        else:
                            send[g * GROUP + j, :, cols] = got_rows[j]
                for m in ms:
                    if m in SELF:
                        continue
                    if g == 0:
                        t_copy(send, m, c).start()
                    elif c == chunks - 1:
                        t_copy(send, m, None).start()
            if c + 2 < chunks:
                x_copy(c + 2).start()

        def landed(m):
            for c in pieces(m):
                t_copy(send, m, c).wait_recv()

        def relay(m):
            landed(m)
            u_copy(m).start()

        swap(0).wait_recv()
        swap(1).wait_recv()
        for p in (1, 2):
            w_up(p).start()
            w_down(p).start()
            w_side(p, 0, core).start()
        for m in RELAYED[:4]:
            relay(m)
        local_w.wait()
        got(0, 0)
        w_up_far(0).start()
        w_side(0, 1, core).start()
        got(1, 0)
        w_down_far(0).start()
        w_side(0, 2, core).start()
        for m in RELAYED[4:]:
            relay(m)
        for p in (1, 2):
            got(0, p)
            w_up_far(p).start()
            w_side(p, 1, core).start()
            got(1, p)
            w_down_far(p).start()
            w_side(p, 2, core).start()

        got(2, 0)
        w_side(0, 3, core).start()
        got(3, 0)
        w_side(0, 4, core).start()
        for n in range(5):
            w_side(0, n, 1 - core).wait_recv()

        for m in SENDS:
            if m not in SELF:
                for c in pieces(m):
                    t_copy(send, m, c).wait_send()

    pl.run_scoped(
        dispatch,
        pltpu.VMEM((peers - 2, padded, width), bf16),
        pltpu.VMEM((2, count, chunk), bf16),
        pltpu.VMEM((peers * padded, count), bf16))

    def finish(wown, wbuf, res, acc, pos):
        flat = jnp.concatenate(
            [pos_a, pos_b, gates[0:1, :], gates[1:2, :], jnp.zeros((124, count), f32)], axis=0)
        pos[...] = flat.T

        step = hidden // 2

        def w_load(q, n, slot):
            cols = pl.ds(n * step, step)
            return pltpu.make_async_copy(held.at[q, :, cols], wbuf.at[slot], wbsem.at[slot])

        def own_load(q):
            return pltpu.make_async_copy(held.at[q], wown.at[q], wosem.at[q])

        def own_product(base, q):
            def one(n, carry):
                cols = pl.ds(pl.multiple_of(n * step, step), step)
                left = recv[base:base + GROUP, 0:span, :].reshape(GROUP * span, width)
                prod = jnp.dot(left, wown[q, :, cols], preferred_element_type=f32).astype(bf16)
                res[base:base + GROUP, 0:span, cols] = prod.reshape(GROUP, span, step)
                return carry

            lax.fori_loop(0, hidden // step, one, 0)

        def partner_product(base, n, slot):
            many = 2 * GROUP
            cols = slice(n * step, (n + 1) * step)
            left = recv[base:base + many, low_rows:padded, :].reshape(many * span, width)
            prod = jnp.dot(left, wbuf[slot], preferred_element_type=f32).astype(bf16)
            prod = prod.reshape(many, span, step)
            edge = res[base:base + many, low_rows:low_rows + 16, cols]
            r = lax.broadcasted_iota(jnp.int32, edge.shape, 1)
            res[base:base + many, low_rows:low_rows + 16, cols] = jnp.where(
                r < cap - low_rows, edge, prod[:, 0:16])
            res[base:base + many, low_rows + 16:padded, cols] = prod[:, 16:]

        def low_copy(m):
            i = SLOTS.index(m)
            return pltpu.make_async_remote_copy(
                src_ref=res.at[i, pl.ds(0, low_rows), :], dst_ref=rr_lo.at[i],
                send_sem=lsend.at[i], recv_sem=lrecv.at[i], device_id={"exp": origin(m)})

        def high_copy(m, n):
            i = SLOTS.index(m)
            cols = pl.ds(n * step, step)
            return pltpu.make_async_remote_copy(
                src_ref=res.at[i, pl.ds(low_rows, sent - low_rows), cols],
                dst_ref=rr_hi.at[i, pl.ds(0, sent - low_rows), cols],
                send_sem=hsend.at[i, n], recv_sem=hrecv.at[i, n], device_id={"exp": origin(m)})

        def arrived(m):
            if m in SELF:
                return
            if m in RELAYED:
                u_copy(m).wait_recv()
            else:
                for c in pieces(m):
                    t_copy(recv, m, c).wait_recv()

        def give_low(base):
            for i in reversed(range(base, base + GROUP)):
                if SLOTS[i] in SELF:
                    rr_lo[i] = res[i, 0:low_rows, :]
                else:
                    low_copy(SLOTS[i]).start()

        def give_high(base, n):
            for i in reversed(range(base, base + 2 * GROUP)):
                if SLOTS[i] in SELF:
                    cols = slice(n * step, (n + 1) * step)
                    rr_hi[i, :, cols] = res[i, low_rows:padded, cols]
                else:
                    high_copy(SLOTS[i], n).start()

        def all_arrived(base):
            for m in SLOTS[base:base + GROUP]:
                arrived(m)

        own_load(0).start()
        own_load(1).start()
        for base, q in ((0, 0), (8, 1)):
            all_arrived(base)
            own_load(q).wait()
            own_product(base, q)
            give_low(base)

        for base, q in ((4, 0), (12, 1)):
            all_arrived(base)
            own_product(base, q)
            give_low(base)

        def far_part(p):
            got(2, p)
            w_side(p, 3, core).start()
            got(3, p)
            w_side(p, 4, core).start()

        def complete(p):
            for n in range(5):
                w_side(p, n, 1 - core).wait_recv()
            for j in range(2):
                w_load(2 + j, p - 1, j).start()

        far_part(1)
        for p in (1, 2):
            complete(p)
            for j in range(2):
                w_load(2 + j, p - 1, j).wait()
                partner_product(8 * j, p - 1, j)
                give_high(8 * j, p - 1)
                if p == 1 and j == 0:
                    far_part(2)

        slot_a, slot_b = pos[:, 0:1], pos[:, 1:2]
        gate_a, gate_b = pos[:, 2:3], pos[:, 3:4]

        def mixed(k, base, high, n):
            size = span if high else low_rows
            lane = lax.broadcasted_iota(jnp.int32, (1, GROUP * size), 1)
            target = jnp.full_like(lane, -1)
            for j in range(GROUP):
                e1, e2 = names_of(SLOTS[base + j])
                local = lane - j * size
                r = local + (low_rows if high else 0)
                value = jnp.where(r < cap, r + e1 * cap, r - cap + e2 * cap)
                target = jnp.where((local >= 0) & (local < size) & (r < rows), value, target)
            target = target.astype(f32)
            mix = jnp.where(slot_a == target, gate_a, 0.0) + jnp.where(slot_b == target, gate_b, 0.0)
            top = mix.astype(bf16)
            rest = (mix - top.astype(f32)).astype(bf16)
            for m in SLOTS[base:base + GROUP]:
                if m not in SELF:
                    (high_copy(m, n) if high else low_copy(m)).wait_recv()
            cols = slice(n * step, (n + 1) * step) if high else slice(0, hidden)
            if high:
                right = rr_hi[base:base + GROUP, :, cols]
                r = lax.broadcasted_iota(jnp.int32, right.shape, 1)
                right = jnp.where(r < rows - low_rows, right, jnp.zeros_like(right))
            else:
                right = rr_lo[base:base + GROUP]
            right = right.reshape(GROUP * size, step if high else hidden)
            part = (jnp.dot(top, right, preferred_element_type=f32)
                    + jnp.dot(rest, right, preferred_element_type=f32))
            if k == 0:
                acc[:, cols] = part
            elif high and base == 8:
                out[:, cols] = (acc[:, cols] + part).astype(bf16)
            else:
                acc[:, cols] += part

        order = [(base, False, 0) for base in (0, 8, 4, 12)]
        order += [(base, True, n) for n in range(2) for base in (4, 0, 12, 8)]
        for k, (base, high, n) in enumerate(order):
            mixed(k, base, high, n)

        for m in SENDS:
            if m not in SELF:
                low_copy(m).wait_send()
                for n in range(2):
                    high_copy(m, n).wait_send()

    pl.run_scoped(
        finish,
        pltpu.VMEM((2, width, hidden), bf16),
        pltpu.VMEM((2, width, hidden // 2), bf16),
        pltpu.VMEM((peers, padded, hidden), bf16),
        pltpu.VMEM((count, hidden), f32),
        pltpu.VMEM((count, 128), f32))

    for m in RELAYED:
        u_copy(m).wait_send()
    swap(0).wait_send()
    swap(1).wait_send()
    for p in range(3):
        for copy in (w_up(p), w_down(p), w_up_far(p), w_down_far(p)):
            copy.wait_send()
        for n in range(5):
            w_side(p, n, core).wait_send()


def body(tokens, routes, gates, weights):
    peers = SIDE * SIDE
    count, width = tokens.shape
    shard, hidden = weights.shape[1:]
    cap = 5 * count // (4 * peers)
    rows = 2 * cap
    padded = -(-rows // 16) * 16
    low_rows = cap // 16 * 16
    span = padded - low_rows
    bf16 = jnp.bfloat16
    dma = pltpu.SemaphoreType.DMA
    vmem = pl.BlockSpec(memory_space=pltpu.VMEM)
    anywhere = pl.BlockSpec(memory_space=pl.ANY)
    mixed, _ = pl.pallas_call(
        functools.partial(kernel, cap),
        out_shape=(
            jax.ShapeDtypeStruct((count, hidden), bf16),
            jax.ShapeDtypeStruct((4, width, hidden), bf16),
        ),
        in_specs=[anywhere, vmem, vmem, anywhere],
        out_specs=(vmem, anywhere),
        scratch_shapes=[
            pltpu.VMEM((peers, padded, width), bf16),
            pltpu.VMEM((len(RELAYED), padded, width), bf16),
            pltpu.VMEM((peers, low_rows, hidden), bf16),
            pltpu.VMEM((peers, span, hidden), bf16),
            dma((2,)),
            dma((2,)),
            dma((2,)),
            dma((peers, 4)),
            dma((peers, 4)),
            dma((len(RELAYED),)),
            dma((len(RELAYED),)),
            dma((peers,)),
            dma((peers,)),
            dma((peers, 2)),
            dma((peers, 2)),
            dma,
            dma((32,)),
            dma((32,)),
        ],
        compiler_params=pltpu.CompilerParams(
            collective_id=0, has_side_effects=True, vmem_limit_bytes=67043328),
    )(tokens, routes.T, gates.T, weights)
    return mixed


def solution(mesh):
    if mesh.shape["exp"] != SIDE * SIDE or mesh.shape["seq"] != 2 * DEPTH:
        raise ValueError("mesh")
    return jax.shard_map(
        body,
        mesh=mesh,
        in_specs=(
            P(("seq", "exp"), None),
            P(("seq", "exp"), None),
            P(("seq", "exp"), None),
            P("exp", "seq", None),
        ),
        out_specs=P(("seq", "exp"), None),
        check_vma=False,
    )
```
